32 devices in a mesh: tg: 4 (over z), pp: 2 (over y), grp: 4 (over x, core).
Axes of the slice: x: 2, y: 2, z: 4, core: 2. Of those that a mesh axis runs over, the one named last changes fastest.
Arguments:
- hidden_in: bfloat16 [512, 1024], P(('pp', 'grp'))
- seq_lens: int32 [512], P(('pp', 'grp'))
- k_cache: bfloat16 [2, 512, 128, 16, 64], P(None, ('pp', 'grp'), None, 'tg')
- v_cache: bfloat16 [2, 512, 128, 16, 64], P(None, ('pp', 'grp'), None, 'tg')
- attn_gain: bfloat16 [2, 1024], P('pp')
- w_qkv: bfloat16 [2, 3072, 1024], P('pp', ('tg', 'grp'))
- w_o: bfloat16 [2, 1024, 1024], P('pp', None, ('tg', 'grp'))
- mlp_gain: bfloat16 [2, 1024], P('pp')
- w_gate_up: bfloat16 [2, 5632, 1024], P('pp', ('tg', 'grp'))
- w_down: bfloat16 [2, 1024, 2816], P('pp', None, ('tg', 'grp'))
Outputs:
- output 1: bfloat16 [512, 1024], P(('pp', 'grp'))
- output 2: bfloat16 [2, 512, 128, 16, 64], P(None, ('pp', 'grp'), None, 'tg')
- output 3: bfloat16 [2, 512, 128, 16, 64], P(None, ('pp', 'grp'), None, 'tg')
- output 4: bfloat16 [2, 3072, 1024], P(None, 'tg')
- output 5: bfloat16 [2, 5632, 1024], P(None, 'tg')
All inputs are finite; a program needn't handle non-finite values.
Results may differ from the reference program's by a relative error of at most 0.0151185.
Values are sent between devices in bfloat16 or wider.
A program may use at most 1 GiB of HBM per device.

```python
import jax
import jax.numpy as jnp
from jax import lax
import math

MODEL_DIM = 1024
FFN_DIM = 2816
HEADS = 16
KV_HEADS = 16
HEAD_DIM = 64
LAYERS = 2
GEN_TP = 4
TRAIN_TP = 16
BATCH = 512
CACHE_LEN = 128

ROPE_THETA = 500000.0
NORM_EPS = 1e-5
MASK_FILL = -1e30


def draw_lens(key):
    key_len, key_top = jax.random.split(key)
    drawn = jax.random.randint(key_len, (BATCH,), CACHE_LEN // 8, CACHE_LEN)
    top_row = jax.random.randint(key_top, (), 0, BATCH)
    return jnp.where(jnp.arange(BATCH) == top_row, CACHE_LEN - 1, drawn).astype(jnp.int32)


def setup_inputs(seed: int = 0) -> dict:
    key_list = jax.random.split(jax.random.key(seed), 11)
    qkv_rows = (HEADS + 2 * KV_HEADS) * HEAD_DIM
    cache_shape = (LAYERS, BATCH, CACHE_LEN, KV_HEADS, HEAD_DIM)
    key_scale = math.sqrt(0.5 * math.log(CACHE_LEN))
    hidden_in = jax.random.normal(key_list[0], (BATCH, MODEL_DIM), jnp.float32)
    seq_lens = draw_lens(key_list[1])
    k_cache = jax.random.normal(key_list[2], cache_shape, jnp.float32) * key_scale
    v_mean = jax.random.normal(key_list[3], (LAYERS, BATCH, 1, KV_HEADS, HEAD_DIM), jnp.float32)
    v_cache = 0.5 * v_mean + jax.random.normal(key_list[4], cache_shape, jnp.float32)
    attn_gain = jax.random.uniform(key_list[5], (LAYERS, MODEL_DIM), jnp.float32, 0.2, 1.8)
    w_qkv = jax.random.normal(key_list[6], (LAYERS, qkv_rows, MODEL_DIM), jnp.float32) * MODEL_DIM ** -0.5
    w_o = jax.random.normal(key_list[7], (LAYERS, MODEL_DIM, HEADS * HEAD_DIM), jnp.float32) * (HEADS * HEAD_DIM) ** -0.5
    mlp_gain = jax.random.uniform(key_list[8], (LAYERS, MODEL_DIM), jnp.float32, 0.5, 1.5)
    w_gate_up = jax.random.normal(key_list[9], (LAYERS, 2 * FFN_DIM, MODEL_DIM), jnp.float32) * MODEL_DIM ** -0.5
    w_down = jax.random.normal(key_list[10], (LAYERS, MODEL_DIM, FFN_DIM), jnp.float32) * FFN_DIM ** -0.5
    return {
        "hidden_in": hidden_in.astype(jnp.bfloat16),
        "seq_lens": seq_lens,
        "k_cache": k_cache.astype(jnp.bfloat16),
        "v_cache": v_cache.astype(jnp.bfloat16),
        "attn_gain": attn_gain.astype(jnp.bfloat16),
        "w_qkv": w_qkv.astype(jnp.bfloat16),
        "w_o": w_o.astype(jnp.bfloat16),
        "mlp_gain": mlp_gain.astype(jnp.bfloat16),
        "w_gate_up": w_gate_up.astype(jnp.bfloat16),
        "w_down": w_down.astype(jnp.bfloat16),
    }


def rms_norm(hidden, gain_vec):
    hidden_f32 = hidden.astype(jnp.float32)
    inv_rms = lax.rsqrt(jnp.mean(hidden_f32 * hidden_f32, axis=-1, keepdims=True) + NORM_EPS)
    return (hidden_f32 * inv_rms * gain_vec.astype(jnp.float32)).astype(jnp.bfloat16)


def apply_rope(values, cos_t, sin_t):
    half_dim = values.shape[-1] // 2
    first_half = values[..., :half_dim]
    second_half = values[..., half_dim:]
    return jnp.concatenate([first_half * cos_t - second_half * sin_t, second_half * cos_t + first_half * sin_t], axis=-1)


def reference(hidden_in, seq_lens, k_cache, v_cache, attn_gain, w_qkv, w_o, mlp_gain, w_gate_up, w_down):
    group_rep = HEADS // KV_HEADS
    blocks = w_qkv.reshape(LAYERS, KV_HEADS, group_rep + 2, HEAD_DIM, MODEL_DIM)
    w_query = blocks[:, :, :group_rep].reshape(LAYERS, HEADS * HEAD_DIM, MODEL_DIM)
    w_key = blocks[:, :, group_rep].reshape(LAYERS, KV_HEADS * HEAD_DIM, MODEL_DIM)
    w_value = blocks[:, :, group_rep + 1].reshape(LAYERS, KV_HEADS * HEAD_DIM, MODEL_DIM)
    gen_qkv = jnp.concatenate([
        w_query.reshape(LAYERS, GEN_TP, -1, MODEL_DIM),
        w_key.reshape(LAYERS, GEN_TP, -1, MODEL_DIM),
        w_value.reshape(LAYERS, GEN_TP, -1, MODEL_DIM)], axis=2).reshape(LAYERS, -1, MODEL_DIM)
    fused_rows = w_gate_up.reshape(LAYERS, TRAIN_TP, 2, FFN_DIM // TRAIN_TP, MODEL_DIM)
    w_gate = fused_rows[:, :, 0].reshape(LAYERS, FFN_DIM, MODEL_DIM)
    w_up = fused_rows[:, :, 1].reshape(LAYERS, FFN_DIM, MODEL_DIM)
    gen_gate_up = jnp.stack([
        w_gate.reshape(LAYERS, GEN_TP, -1, MODEL_DIM),
        w_up.reshape(LAYERS, GEN_TP, -1, MODEL_DIM)], axis=2).reshape(LAYERS, 2 * FFN_DIM, MODEL_DIM)

    positions = jnp.arange(CACHE_LEN)
    row_ids = jnp.arange(BATCH)
    inv_freq = jnp.power(ROPE_THETA, -jnp.arange(0, HEAD_DIM, 2).astype(jnp.float32) / HEAD_DIM)
    angles = seq_lens.astype(jnp.float32)[:, None] * inv_freq[None, :]
    cos_t = jnp.cos(angles)[:, None, :]
    sin_t = jnp.sin(angles)[:, None, :]
    score_scale = HEAD_DIM ** -0.5

    def attend_row(row_args):
        query_row, k_row, v_row, length = row_args
        query_grp = query_row.reshape(KV_HEADS, group_rep, HEAD_DIM).astype(jnp.float32)
        scores = jnp.einsum("grd,sgd->grs", query_grp, k_row.astype(jnp.float32)) * score_scale
        scores = jnp.where(positions[None, None, :] <= length, scores, MASK_FILL)
        attn_probs = jax.nn.softmax(scores, axis=-1).astype(jnp.bfloat16)
        out_row = jnp.einsum("grs,sgd->grd", attn_probs.astype(jnp.float32), v_row.astype(jnp.float32))
        return out_row.astype(jnp.bfloat16).reshape(HEADS * HEAD_DIM)

    def layer_step(hidden, layer_xs):
        gain_attn, wgt_query, wgt_key, wgt_value, wgt_out, gain_mlp, wgt_gate, wgt_up, wgt_down, k_layer, v_layer = layer_xs
        normed = rms_norm(hidden, gain_attn)
        query_vals = jnp.dot(normed, wgt_query.T, preferred_element_type=jnp.float32).reshape(BATCH, HEADS, HEAD_DIM)
        key_new = jnp.dot(normed, wgt_key.T, preferred_element_type=jnp.float32).reshape(BATCH, KV_HEADS, HEAD_DIM)
        value_new = jnp.dot(normed, wgt_value.T, preferred_element_type=jnp.float32).reshape(BATCH, KV_HEADS, HEAD_DIM).astype(jnp.bfloat16)
        query_vals = apply_rope(query_vals, cos_t, sin_t).astype(jnp.bfloat16)
        key_new = apply_rope(key_new, cos_t, sin_t).astype(jnp.bfloat16)
        k_layer = k_layer.at[row_ids, seq_lens].set(key_new)
        v_layer = v_layer.at[row_ids, seq_lens].set(value_new)
        attn_out = lax.map(attend_row, (query_vals, k_layer, v_layer, seq_lens))
        attn_proj = jnp.dot(attn_out, wgt_out.T, preferred_element_type=jnp.float32)
        hidden = (hidden.astype(jnp.float32) + attn_proj).astype(jnp.bfloat16)
        normed = rms_norm(hidden, gain_mlp)
        gate_vals = jnp.dot(normed, wgt_gate.T, preferred_element_type=jnp.float32)
        up_vals = jnp.dot(normed, wgt_up.T, preferred_element_type=jnp.float32)
        act_vals = (jax.nn.silu(gate_vals) * up_vals).astype(jnp.bfloat16)
        down_vals = jnp.dot(act_vals, wgt_down.T, preferred_element_type=jnp.float32)
        hidden = (hidden.astype(jnp.float32) + down_vals).astype(jnp.bfloat16)
        return hidden, (k_layer, v_layer)

    layer_xs = (attn_gain, w_query, w_key, w_value, w_o, mlp_gain, w_gate, w_up, w_down, k_cache, v_cache)
    hidden_out, cache_pair = lax.scan(layer_step, hidden_in, layer_xs)
    return (hidden_out, cache_pair[0], cache_pair[1], gen_qkv, gen_gate_up)
```

```python
import functools

import jax
import jax.numpy as jnp
from jax import lax
from jax.experimental import pallas as pl
from jax.experimental.pallas import tpu as pltpu
from jax.sharding import PartitionSpec as P

ROPE_THETA = 500000.0
NORM_EPS = 1e-5
MASK_FILL = -1e30
ROW_AXES = ("pp", "grp")
TRAIN_AXES = ("tg", "grp")
BF16 = jnp.bfloat16
F32 = jnp.float32
MESH = pl.DeviceIdType.MESH
ANY = pl.BlockSpec(memory_space=pl.ANY)
VMEM = pl.BlockSpec(memory_space=pltpu.VMEM)
SEQ_TILE = 16
HEAD_ROWS = 8


def norm_rows(hidden_f32, gain_row):
    inv_rms = lax.rsqrt(jnp.mean(hidden_f32 * hidden_f32, axis=-1, keepdims=True) + NORM_EPS)
    return (hidden_f32 * inv_rms * gain_row).astype(BF16)


def rows(ref, start, count):
    return ref.at[pl.ds(pl.multiple_of(start, 16), count), :]


class Place:
    def __init__(self, tg_size):
        self.tg_size = tg_size
        self.tg = lax.axis_index("tg")
        self.pp = lax.axis_index("pp")
        self.grp = lax.axis_index("grp")
        self.partner = self.grp + 1 - 2 * lax.rem(self.grp, 2)
        self.across = lax.rem(self.grp + 2, 4)
        self.diagonal = lax.rem(self.partner + 2, 4)
        self.stage = 1 - self.pp

    def tg_at(self, step):
        return lax.rem(self.tg + step, self.tg_size)

    def barrier(self, with_tg):
        sem = pltpu.get_barrier_semaphore()
        targets = [{"grp": self.partner}, {"grp": self.across}, {"pp": self.stage}]
        if with_tg:
            targets += [{"tg": self.tg_at(step)} for step in range(1, self.tg_size)]
        for target in targets:
            pl.semaphore_signal(sem, inc=1, device_id=target, device_id_type=MESH)
        pl.semaphore_wait(sem, len(targets))


def gather_sems(count):
    dma = pltpu.SemaphoreType.DMA
    return [dma((count,)), dma((count, 2)), dma((count, 2)), dma((count, 2, 2))]


class Gather:
    def __init__(self, place, sems, index, layer, own, buf, base, stride, count):
        self.place, self.layer, self.own, self.buf = place, layer, own, buf
        self.base, self.stride, self.count = base, stride, count
        local, ysem, xsem, psem = sems
        self.local = local.at[index]
        self.ysem = (ysem.at[index, 0], ysem.at[index, 1])
        self.xsem = (xsem.at[index, 0], xsem.at[index, 1])
        self.psem = [(psem.at[index, k, 0], psem.at[index, k, 1]) for k in range(2)]

    def at(self, grp):
        return rows(self.buf, self.base + grp * self.stride, self.count)

    def remote(self, src, grp, sems, target):
        return pltpu.make_async_remote_copy(
            src_ref=src, dst_ref=self.at(grp), send_sem=sems[0], recv_sem=sems[1],
            device_id=target, device_id_type=MESH)

    def local_copy(self):
        return pltpu.make_async_copy(self.own, self.at(self.place.grp), self.local)

    def y_copy(self):
        return self.remote(self.own, self.place.grp, self.ysem, {"pp": self.place.stage})

    def x_copy(self, grp):
        return self.remote(self.at(grp), grp, self.xsem, {"grp": self.place.across})

    def p_copy(self, grp, which):
        return self.remote(self.at(grp), grp, self.psem[which], {"grp": self.place.partner})

    def start(self):
        @pl.when(self.place.pp == self.layer)
        def _():
            self.y_copy().start()
            self.local_copy().start()

    def send(self):
        @pl.when(self.place.pp == self.layer)
        def _():
            self.local_copy().wait()

        @pl.when(self.place.pp != self.layer)
        def _():
            self.y_copy().wait_recv()

        self.x_copy(self.place.grp).start()
        self.p_copy(self.place.grp, 0).start()

    def forward(self):
        self.x_copy(self.place.across).wait_recv()
        self.p_copy(self.place.across, 1).start()

    def arrive(self):
        self.p_copy(self.place.partner, 0).wait_recv()
        self.p_copy(self.place.diagonal, 1).wait_recv()

    def finish(self):
        @pl.when(self.place.pp == self.layer)
        def _():
            self.y_copy().wait_send()

        self.x_copy(self.place.grp).wait_send()
        self.p_copy(self.place.grp, 0).wait_send()
        self.p_copy(self.place.across, 1).wait_send()


def each(units, what):
    for unit in units:
        getattr(unit, what)()


def row_blocks(kind, sizes):
    head_rows, ffn_rows, merge = sizes
    top = (ffn_rows // 2 + 15) // 16 * 16
    halves = [(0, top), (top, ffn_rows - top)]
    if kind == "qkv":
        return [(k * head_rows, k * merge * head_rows, head_rows, head_rows) for k in range(3)]
    if kind == "o":
        return [(0, 0, head_rows, head_rows)]
    if kind == "gate":
        return [(off, off, ffn_rows, count) for off, count in halves]
    if kind == "up":
        return [(ffn_rows + off, off, ffn_rows, count) for off, count in halves]
    return [(off, off, ffn_rows, count) for off, count in halves]


class SumOverTg:
    def __init__(self, place, part, slots, full, sems):
        self.place, self.part, self.slots, self.full = place, part, slots, full
        self.count = slots.shape[1]
        self.send, self.recv = sems

    def scatter_copy(self, step):
        peer = self.place.tg_at(step)
        return pltpu.make_async_remote_copy(
            src_ref=rows(self.part, peer * self.count, self.count), dst_ref=self.slots.at[step - 1],
            send_sem=self.send.at[0, step - 1], recv_sem=self.recv.at[0, step - 1],
            device_id={"tg": peer}, device_id_type=MESH)

    def spread_copy(self, step):
        own = rows(self.full, self.place.tg * self.count, self.count)
        return pltpu.make_async_remote_copy(
            src_ref=own, dst_ref=own,
            send_sem=self.send.at[1, step - 1], recv_sem=self.recv.at[1, step - 1],
            device_id={"tg": self.place.tg_at(step)}, device_id_type=MESH)

    def spread_wait(self, step):
        peer = self.place.tg_at(self.place.tg_size - step)
        block = rows(self.full, peer * self.count, self.count)
        pltpu.make_async_remote_copy(
            src_ref=block, dst_ref=block,
            send_sem=self.send.at[1, step - 1], recv_sem=self.recv.at[1, step - 1],
            device_id={"tg": peer}, device_id_type=MESH).wait_recv()

    def steps(self):
        return range(1, self.place.tg_size)

    def scatter_start(self):
        for step in self.steps():
            self.scatter_copy(step).start()

    def total(self):
        for step in self.steps():
            self.scatter_copy(step).wait_recv()
        out = self.part[pl.ds(pl.multiple_of(self.place.tg * self.count, self.count), self.count), :]
        for step in self.steps():
            out = out + self.slots[step - 1]
        return out

    def spread_start(self, block):
        self.full[pl.ds(pl.multiple_of(self.place.tg * self.count, self.count), self.count), :] = block
        for step in self.steps():
            self.scatter_copy(step).wait_send()
        for step in self.steps():
            self.spread_copy(step).start()

    def spread_finish(self):
        for step in self.steps():
            self.spread_wait(step)
        for step in self.steps():
            self.spread_copy(step).wait_send()


def dot_nt(lhs, rhs):
    return lax.dot_general(lhs, rhs, (((1,), (1,)), ((), ())), preferred_element_type=F32)


def dot_nn(lhs, rhs):
    return jnp.dot(lhs, rhs, preferred_element_type=F32)


def first_kernel(tg_size, sizes, hidden, attn_gain, mlp_gain, w_qkv, normed, gains, qkv_out,
                 qkv_buf, other_attn, other_mlp, gain_send, gain_recv, out_sem, *sems):
    place = Place(tg_size)
    units = [Gather(place, sems, k, 0, w_qkv.at[pl.ds(src, count), :], qkv_buf, base, stride, count)
             for k, (src, base, stride, count) in enumerate(row_blocks("qkv", sizes))]
    place.barrier(False)
    gain_copies = [
        pltpu.make_async_remote_copy(
            src_ref=src, dst_ref=dst, send_sem=gain_send.at[k], recv_sem=gain_recv.at[k],
            device_id={"pp": place.stage}, device_id_type=MESH)
        for k, (src, dst) in enumerate([(attn_gain, other_attn), (mlp_gain, other_mlp)])]
    for copy in gain_copies:
        copy.start()
    each(units, "start")
    for copy in gain_copies:
        copy.wait()
    first = place.pp == 0
    table = []
    for mine, other in [(attn_gain, other_attn), (mlp_gain, other_mlp)]:
        own_row, far_row = mine[...].astype(F32), other[...].astype(F32)
        table.append(jnp.where(first, own_row, far_row))
        table.append(jnp.where(first, far_row, own_row))
    for k, row in enumerate(table):
        gains[pl.ds(k, 1), :] = row
    normed[...] = norm_rows(hidden[...].astype(F32), table[0])
    each(units, "send")
    each(units, "forward")
    each(units, "arrive")
    copy = pltpu.make_async_copy(qkv_buf, qkv_out, out_sem)
    copy.start()
    each(units, "finish")
    copy.wait()


def attend_kernel(lens, normed, w_qkv, cos_t, sin_t, k_in, v_in, *rest, head_dim, aliased):
    if aliased:
        rest = rest[2:]
    k_out, v_out, attn_out, q_scr, k_scr, v_scr = rest
    batch = normed.shape[0]
    width = q_scr.shape[1]
    heads = width // head_dim
    half = head_dim // 2
    cache_len = k_in.shape[3]
    step = pl.program_id(0)

    @pl.when(step == 0)
    def _():
        proj = dot_nt(w_qkv[...], normed[...])
        cos_v, sin_v = cos_t[...], sin_t[...]

        def rope(block):
            pieces = []
            for head in range(heads):
                first = block[head * head_dim:head * head_dim + half]
                second = block[head * head_dim + half:(head + 1) * head_dim]
                pieces += [first * cos_v - second * sin_v, second * cos_v + first * sin_v]
            return jnp.concatenate(pieces, axis=0).astype(BF16).astype(F32)

        q_scr[...] = jnp.transpose(rope(proj[:width])) * (head_dim ** -0.5)
        pad = jnp.zeros((width, cache_len - batch), F32)
        k_scr[...] = jnp.concatenate([rope(proj[width:2 * width]), pad], axis=1)
        v_scr[...] = jnp.concatenate([proj[2 * width:].astype(BF16).astype(F32), pad], axis=1)

    seq0 = step * SEQ_TILE
    shift = lax.rem(cache_len - seq0, cache_len)
    k_cols = pltpu.roll(k_scr[...], shift, 1)
    v_cols = pltpu.roll(v_scr[...], shift, 1)
    lane = lax.broadcasted_iota(jnp.int32, (width, cache_len), 1)
    own_head = (lax.broadcasted_iota(jnp.int32, (HEAD_ROWS, width), 1) // head_dim
                == lax.broadcasted_iota(jnp.int32, (HEAD_ROWS, width), 0))
    lane_row = lax.broadcasted_iota(jnp.int32, (HEAD_ROWS, cache_len), 1)
    scores = []
    for j in range(SEQ_TILE):
        length = lens[seq0 + j]
        k_new = jnp.where(lane == length, k_cols[:, j:j + 1], k_in[0, j].astype(F32)).astype(BF16)
        k_out[0, j] = k_new
        q_block = jnp.where(own_head, q_scr[pl.ds(seq0 + j, 1), :], 0.0).astype(BF16)
        score = dot_nn(q_block, k_new)
        scores.append(jnp.where(lane_row <= length, score, MASK_FILL))
    score = jnp.concatenate(scores, axis=0)
    expo = jnp.exp(score - jnp.max(score, axis=-1, keepdims=True))
    probs = (expo / jnp.sum(expo, axis=-1, keepdims=True)).astype(BF16)
    outs = []
    for j in range(SEQ_TILE):
        length = lens[seq0 + j]
        v_new = jnp.where(lane == length, v_cols[:, j:j + 1], v_in[0, j].astype(F32)).astype(BF16)
        v_out[0, j] = v_new
        mixed = dot_nt(probs[j * HEAD_ROWS:(j + 1) * HEAD_ROWS], v_new)
        outs.append(jnp.sum(jnp.where(own_head, mixed, 0.0), axis=0, keepdims=True))
    attn_out[...] = jnp.concatenate(outs, axis=0).astype(BF16)


def attend(layer, lens, normed, w_qkv, cos_t, sin_t, k_cache, v_cache, prior, head_dim):
    layers, batch, width, cache_len = k_cache.shape
    tile = pl.BlockSpec((1, SEQ_TILE, width, cache_len), lambda i, *_: (layer, i, 0, 0))
    whole = lambda arr: pl.BlockSpec(arr.shape, lambda i, *_: (0,) * arr.ndim)
    aliased = prior is not None
    operands = [normed, w_qkv, cos_t, sin_t, k_cache, v_cache]
    in_specs = [whole(normed), whole(w_qkv), whole(cos_t), whole(sin_t), tile, tile]
    aliases = {}
    if aliased:
        operands += list(prior)
        in_specs += [ANY, ANY]
        aliases = {7: 0, 8: 1}
    flat = jax.ShapeDtypeStruct(k_cache.shape, BF16)
    return pl.pallas_call(
        functools.partial(attend_kernel, head_dim=head_dim, aliased=aliased),
        grid_spec=pltpu.PrefetchScalarGridSpec(
            num_scalar_prefetch=1, grid=(batch // SEQ_TILE,), in_specs=in_specs,
            out_specs=[tile, tile, pl.BlockSpec((SEQ_TILE, width), lambda i, *_: (i, 0))],
            scratch_shapes=[pltpu.VMEM((batch, width), F32), pltpu.VMEM((width, cache_len), F32),
                            pltpu.VMEM((width, cache_len), F32)]),
        out_shape=[flat, flat, jax.ShapeDtypeStruct((batch, width), BF16)],
        input_output_aliases=aliases,
        name=f"attend_{layer}",
    )(lens, *operands)


def first_layer_kernel(tg_size, sizes, attn, hidden, gains, w_qkv, w_o, w_gu, w_dn,
                       normed, h_out, gu0_out, qkv1, o1, gate1,
                       o_buf, gate_buf, up_buf, dn_buf, part, slots, mid, gu_sem, sum_send, sum_recv,
                       *sems):
    place = Place(tg_size)
    index = [0]

    def make(kind, layer, src_ref, buf):
        out = []
        for src, base, stride, count in row_blocks(kind, sizes):
            out.append(Gather(place, sems, index[0], layer, src_ref.at[pl.ds(src, count), :], buf,
                              base, stride, count))
            index[0] += 1
        return out

    o_u = make("o", 0, w_o, o_buf)
    gate_u = make("gate", 0, w_gu, gate_buf)
    up_u = make("up", 0, w_gu, up_buf)
    dn_u = make("dn", 0, w_dn, dn_buf)
    next_u = make("qkv", 1, w_qkv, qkv1) + make("o", 1, w_o, o1) + make("gate", 1, w_gu, gate1)
    every = o_u + gate_u + up_u + dn_u + next_u
    sum_o = SumOverTg(place, part.at[0], slots.at[0], mid, (sum_send.at[0], sum_recv.at[0]))
    sum_d = SumOverTg(place, part.at[1], slots.at[1], normed, (sum_send.at[1], sum_recv.at[1]))
    count = slots.shape[2]
    own = pl.ds(pl.multiple_of(place.tg * count, count), count)
    ffn = gate_buf.shape[0]

    place.barrier(True)
    each(every, "start")
    o_u[0].send()
    gate_u[0].send()
    o_u[0].forward()
    o_u[0].arrive()
    part[0] = dot_nn(attn[...], o_buf[...])
    sum_o.scatter_start()
    gate_u[1].send()
    gate_u[0].forward()
    up_u[0].send()
    gate_u[1].forward()
    h_mid = (hidden[own, :].astype(F32) + sum_o.total()).astype(BF16).astype(F32)
    sum_o.spread_start(norm_rows(h_mid, gains[2:3, :]))
    up_u[1].send()
    up_u[0].forward()
    sum_o.spread_finish()
    each(gate_u, "arrive")
    act_in = mid[...]
    gate = dot_nt(act_in, gate_buf[...])
    gate = jax.nn.silu(gate)
    dn_u[0].send()
    up_u[1].forward()
    each(up_u, "arrive")
    gate_out_copy = pltpu.make_async_copy(gate_buf, gu0_out.at[pl.ds(0, ffn), :], gu_sem.at[0])
    up_out_copy = pltpu.make_async_copy(up_buf, gu0_out.at[pl.ds(ffn, ffn), :], gu_sem.at[1])
    gate_out_copy.start()
    up_out_copy.start()
    act = (gate * dot_nt(act_in, up_buf[...])).astype(BF16)
    dn_u[1].send()
    each(next_u[:2], "send")
    each(dn_u, "forward")
    each(dn_u, "arrive")
    part[1] = dot_nn(act, dn_buf[...])
    sum_d.scatter_start()
    each(next_u[2:], "send")
    each(next_u[:2], "forward")
    h_new = (h_mid + sum_d.total()).astype(BF16)
    h_out[...] = h_new
    sum_d.spread_start(norm_rows(h_new.astype(F32), gains[1:2, :]))
    each(next_u[2:], "forward")
    sum_d.spread_finish()
    each(next_u, "arrive")
    each(every, "finish")
    gate_out_copy.wait()
    up_out_copy.wait()


def last_layer_kernel(tg_size, sizes, attn, h_in, gains, o1, gate1, w_gu, w_dn,
                      hidden_out, up1_out,
                      up_buf, dn_buf, part, slots, mid, up_sem, sum_send, sum_recv, *sems):
    place = Place(tg_size)
    index = [0]

    def make(kind, layer, src_ref, buf):
        out = []
        for src, base, stride, count in row_blocks(kind, sizes):
            out.append(Gather(place, sems, index[0], layer, src_ref.at[pl.ds(src, count), :], buf,
                              base, stride, count))
            index[0] += 1
        return out

    up_u = make("up", 1, w_gu, up_buf)
    dn_u = make("dn", 1, w_dn, dn_buf)
    every = up_u + dn_u
    sum_o = SumOverTg(place, part.at[0], slots.at[0], mid, (sum_send.at[0], sum_recv.at[0]))
    sum_d = SumOverTg(place, part.at[1], slots.at[1], hidden_out, (sum_send.at[1], sum_recv.at[1]))

    place.barrier(True)
    each(every, "start")
    part[0] = dot_nn(attn[...], o1[...])
    sum_o.scatter_start()
    each(up_u, "send")
    dn_u[0].send()
    up_u[0].forward()
    h_mid = (h_in[...].astype(F32) + sum_o.total()).astype(BF16).astype(F32)
    sum_o.spread_start(norm_rows(h_mid, gains[3:4, :]))
    dn_u[1].send()
    up_u[1].forward()
    sum_o.spread_finish()
    act_in = mid[...]
    gate = jax.nn.silu(dot_nt(act_in, gate1[...]))
    each(dn_u, "forward")
    each(up_u, "arrive")
    up_out_copy = pltpu.make_async_copy(up_buf, up1_out, up_sem)
    up_out_copy.start()
    act = (gate * dot_nt(act_in, up_buf[...])).astype(BF16)
    each(dn_u, "arrive")
    part[1] = dot_nn(act, dn_buf[...])
    sum_d.scatter_start()
    h_new = (h_mid + sum_d.total()).astype(BF16)
    sum_d.spread_start(h_new)
    each(every, "finish")
    up_out_copy.wait()
    sum_d.spread_finish()


def remote_params(collective_id):
    return pltpu.CompilerParams(collective_id=collective_id, has_side_effects=True,
                                vmem_limit_bytes=48 * 1024 * 1024)


def solution(mesh):
    merge = mesh.shape["grp"]
    tg_size = mesh.shape["tg"]
    cache_spec = P(None, ROW_AXES, None, "tg", None)
    in_specs = (P(ROW_AXES, None), P(ROW_AXES), cache_spec, cache_spec,
                P("pp", None), P("pp", TRAIN_AXES, None), P("pp", None, TRAIN_AXES),
                P("pp", None), P("pp", TRAIN_AXES, None), P("pp", None, TRAIN_AXES))
    out_specs = (P(ROW_AXES, None), cache_spec, cache_spec, P(None, "tg", None), P(None, "tg", None))

    def body(hidden_in, seq_lens, k_cache, v_cache, attn_gain, w_qkv, w_o, mlp_gain, w_gate_up, w_down):
        batch, dim = hidden_in.shape
        layers, _, cache_len, kv_loc, head_dim = k_cache.shape
        width = kv_loc * head_dim
        ffn_rows = w_gate_up.shape[1] // 2
        ffn = ffn_rows * merge
        sizes = (head_dim, ffn_rows, merge)
        quarter = batch // tg_size
        w_qkv, w_gate_up = w_qkv[0], w_gate_up[0]
        w_o_t, w_down_t = jnp.transpose(w_o[0]), jnp.transpose(w_down[0])
        flat = lambda cache: jnp.transpose(cache, (0, 1, 3, 4, 2)).reshape(layers, batch, width, cache_len)
        k_flat, v_flat = flat(k_cache), flat(v_cache)
        inv_freq = jnp.power(ROPE_THETA, -jnp.arange(0, head_dim, 2).astype(F32) / head_dim)
        angles = inv_freq[:, None] * seq_lens.astype(F32)[None, :]
        cos_t, sin_t = jnp.cos(angles), jnp.sin(angles)
        dma = pltpu.SemaphoreType.DMA
        sds = jax.ShapeDtypeStruct

        normed, gains, qkv0 = pl.pallas_call(
            functools.partial(first_kernel, tg_size, sizes),
            in_specs=[VMEM, VMEM, VMEM, ANY], out_specs=[VMEM, VMEM, ANY],
            out_shape=[sds((batch, dim), BF16), sds((4, dim), F32), sds((3 * width, dim), BF16)],
            scratch_shapes=[pltpu.VMEM((3 * width, dim), BF16), pltpu.VMEM((1, dim), BF16),
                            pltpu.VMEM((1, dim), BF16), dma((2,)), dma((2,)), dma(())] + gather_sems(3),
            compiler_params=remote_params(1), name="first",
        )(hidden_in, attn_gain, mlp_gain, w_qkv)

        k_out, v_out, attn = attend(0, seq_lens, normed, qkv0, cos_t, sin_t, k_flat, v_flat, None, head_dim)

        normed, h_own, gu0, qkv1, o1, gate1 = pl.pallas_call(
            functools.partial(first_layer_kernel, tg_size, sizes),
            in_specs=[VMEM, VMEM, VMEM, ANY, ANY, ANY, ANY],
            out_specs=[VMEM, VMEM, ANY, ANY, ANY, ANY],
            out_shape=[sds((batch, dim), BF16), sds((quarter, dim), BF16), sds((2 * ffn, dim), BF16),
                       sds((3 * width, dim), BF16), sds((width, dim), BF16), sds((ffn, dim), BF16)],
            scratch_shapes=[pltpu.VMEM((width, dim), BF16), pltpu.VMEM((ffn, dim), BF16),
                            pltpu.VMEM((ffn, dim), BF16), pltpu.VMEM((ffn, dim), BF16),
                            pltpu.VMEM((2, batch, dim), F32), pltpu.VMEM((2, tg_size - 1, quarter, dim), F32),
                            pltpu.VMEM((batch, dim), BF16), dma((2,)),
                            dma((2, 2, tg_size - 1)), dma((2, 2, tg_size - 1))] + gather_sems(13),
            compiler_params=remote_params(2), name="layer_0",
        )(attn, hidden_in, gains, w_qkv, w_o_t, w_gate_up, w_down_t)

        k_out, v_out, attn = attend(1, seq_lens, normed, qkv1, cos_t, sin_t, k_flat, v_flat,
                                    (k_out, v_out), head_dim)

        hidden, up1 = pl.pallas_call(
            functools.partial(last_layer_kernel, tg_size, sizes),
            in_specs=[VMEM, VMEM, VMEM, VMEM, VMEM, ANY, ANY],
            out_specs=[VMEM, ANY],
            out_shape=[sds((batch, dim), BF16), sds((ffn, dim), BF16)],
            scratch_shapes=[pltpu.VMEM((ffn, dim), BF16), pltpu.VMEM((ffn, dim), BF16),
                            pltpu.VMEM((2, batch, dim), F32), pltpu.VMEM((2, tg_size - 1, quarter, dim), F32),
                            pltpu.VMEM((batch, dim), BF16), dma(()),
                            dma((2, 2, tg_size - 1)), dma((2, 2, tg_size - 1))] + gather_sems(4),
            compiler_params=remote_params(3), name="layer_1",
        )(attn, h_own, gains, o1, gate1, w_gate_up, w_down_t)

        unflat = lambda cache: jnp.transpose(
            cache.reshape(layers, batch, kv_loc, head_dim, cache_len), (0, 1, 4, 2, 3))
        gen_qkv = jnp.stack([qkv0, qkv1])
        gen_gate_up = jnp.stack([gu0, jnp.concatenate([gate1, up1], axis=0)])
        return hidden, unflat(k_out), unflat(v_out), gen_qkv, gen_gate_up

    return jax.shard_map(body, mesh=mesh, in_specs=in_specs, out_specs=out_specs, check_vma=False)
```

```python
import functools
import math

import jax
import jax.numpy as jnp
from jax import lax
from jax.experimental import pallas as pl
from jax.experimental.pallas import tpu as pltpu
from jax.sharding import PartitionSpec as P

ROPE_THETA = 500000.0
NORM_EPS = 1e-5
MASK_FILL = -1e30
ROW_AXES = ("pp", "grp")
TRAIN_AXES = ("tg", "grp")
BF16 = jnp.bfloat16
F32 = jnp.float32
MESH = pl.DeviceIdType.MESH
HBM = pl.BlockSpec(memory_space=pltpu.HBM)
SMEM = pl.BlockSpec(memory_space=pltpu.SMEM)
VMEM = pl.BlockSpec(memory_space=pltpu.VMEM)
SEQ_TILE = 16
HEAD_ROWS = 8


def norm_rows(hidden_f32, gain_row):
    inv_rms = lax.rsqrt(jnp.mean(hidden_f32 * hidden_f32, axis=-1, keepdims=True) + NORM_EPS)
    return (hidden_f32 * inv_rms * gain_row).astype(BF16)


def rows(ref, start, count):
    return ref.at[pl.ds(pl.multiple_of(start, 16), count), :]


class Place:
    def __init__(self, tg_size):
        self.tg_size = tg_size
        self.tg = lax.axis_index("tg")
        self.pp = lax.axis_index("pp")
        self.grp = lax.axis_index("grp")
        self.partner = self.grp + 1 - 2 * lax.rem(self.grp, 2)
        self.across = lax.rem(self.grp + 2, 4)
        self.diagonal = lax.rem(self.partner + 2, 4)
        self.stage = 1 - self.pp

    def tg_at(self, step):
        return lax.rem(self.tg + step, self.tg_size)

    def barrier(self, with_tg):
        sem = pltpu.get_barrier_semaphore()
        targets = [{"grp": self.partner}, {"grp": self.across}, {"pp": self.stage}]
        if with_tg:
            targets += [{"tg": self.tg_at(step)} for step in range(1, self.tg_size)]
        for target in targets:
            pl.semaphore_signal(sem, inc=1, device_id=target, device_id_type=MESH)
        pl.semaphore_wait(sem, len(targets))


def gather_sems(count):
    dma = pltpu.SemaphoreType.DMA
    return [dma((count,)), dma((count, 2)), dma((count, 2)), dma((count, 2)), dma((count, 2, 2))]


class Cross:
    def __init__(self, place, sems, index, layer, own, held):
        self.place, self.layer = place, layer
        self.copy = lambda: pltpu.make_async_remote_copy(
            src_ref=own, dst_ref=held, send_sem=sems[1].at[index, 0], recv_sem=sems[1].at[index, 1],
            device_id={"pp": place.stage}, device_id_type=MESH)

    def start(self):
        @pl.when(self.place.pp == self.layer)
        def _():
            self.copy().start()

    def finish(self):
        @pl.when(self.place.pp == self.layer)
        def _():
            self.copy().wait_send()

        @pl.when(self.place.pp != self.layer)
        def _():
            self.copy().wait_recv()


class Gather:
    def __init__(self, place, sems, index, layer, own, held, buf, base, stride, count, route):
        self.place, self.layer, self.own, self.held, self.buf = place, layer, own, held, buf
        self.base, self.stride, self.count, self.route = base, stride, count, route
        local, ysem, zsem, xsem, psem = sems
        self.local = local.at[index]
        self.ysem = (ysem.at[index, 0], ysem.at[index, 1])
        self.zsem = (zsem.at[index, 0], zsem.at[index, 1])
        self.xsem = (xsem.at[index, 0], xsem.at[index, 1])
        self.psem = [(psem.at[index, k, 0], psem.at[index, k, 1]) for k in range(2)]

    def on(self, owner, body):
        pl.when(self.place.pp == self.layer if owner else self.place.pp != self.layer)(body)

    def at(self, grp):
        return rows(self.buf, self.base + grp * self.stride, self.count)

    def remote(self, src, grp, sems, target):
        return pltpu.make_async_remote_copy(
            src_ref=src, dst_ref=self.at(grp), send_sem=sems[0], recv_sem=sems[1],
            device_id=target, device_id_type=MESH)

    def local_copy(self, src):
        return pltpu.make_async_copy(src, self.at(self.place.grp), self.local)

    def y_copy(self):
        return self.remote(self.own, self.place.grp, self.ysem, {"pp": self.place.stage})

    def z_copy(self):
        grp = self.place.across
        return self.remote(self.at(grp), grp, self.zsem, {"pp": self.place.stage})

    def x_copy(self, grp):
        return self.remote(self.at(grp), grp, self.xsem, {"grp": self.place.across})

    def p_copy(self, grp, which):
        return self.remote(self.at(grp), grp, self.psem[which], {"grp": self.place.partner})

    def start(self):
        def owner():
            if self.held is None:
                self.y_copy().start()
            self.local_copy(self.own).start()

        self.on(True, owner)
        if self.held is not None:
            self.on(False, lambda: self.local_copy(self.held).start())

    def send(self):
        self.on(True, lambda: self.local_copy(self.own).wait())
        if self.held is None:
            self.on(False, lambda: self.y_copy().wait_recv())
        else:
            self.on(False, lambda: self.local_copy(self.held).wait())
        grp = self.place.grp
        if self.route == "both":
            self.x_copy(grp).start()
        else:
            self.on(self.route == "owner", lambda: self.x_copy(grp).start())
        self.p_copy(grp, 0).start()

    def forward(self):
        grp = self.place.across
        if self.route == "both":
            self.x_copy(grp).wait_recv()
        else:
            def relay():
                self.x_copy(grp).wait_recv()
                self.z_copy().start()

            self.on(self.route == "owner", relay)
            self.on(self.route != "owner", lambda: self.z_copy().wait_recv())
        self.p_copy(grp, 1).start()

    def arrive(self):
        self.p_copy(self.place.partner, 0).wait_recv()
        self.p_copy(self.place.diagonal, 1).wait_recv()

    def finish(self):
        if self.held is None:
            self.on(True, lambda: self.y_copy().wait_send())
        grp = self.place.grp
        if self.route == "both":
            self.x_copy(grp).wait_send()
        else:
            def relayed():
                self.x_copy(grp).wait_send()
                self.z_copy().wait_send()

            self.on(self.route == "owner", relayed)
        self.p_copy(grp, 0).wait_send()
        self.p_copy(self.place.across, 1).wait_send()


class Maker:
    def __init__(self, place, sems, sizes):
        self.place, self.sems, self.sizes, self.index = place, sems, sizes, 0

    def gather(self, kind, layer, src_ref, buf, routes, held=None):
        out = []
        for (src, hold, base, stride, count), route in zip(row_blocks(kind, self.sizes), routes, strict=True):
            out.append(Gather(self.place, self.sems, self.index, layer, src_ref.at[pl.ds(src, count), :],
                              None if held is None else held.at[pl.ds(hold, count), :],
                              buf, base, stride, count, route))
            self.index += 1
        return out

    def cross(self, kind, layer, src_ref, held):
        out = []
        for src, hold, _, _, count in row_blocks(kind, self.sizes):
            out.append(Cross(self.place, self.sems, self.index, layer, src_ref.at[pl.ds(src, count), :],
                             held.at[pl.ds(hold, count), :]))
            self.index += 1
        return out


def each(units, what):
    for unit in units:
        getattr(unit, what)()


def row_blocks(kind, sizes):
    head_rows, ffn_rows, merge = sizes
    top = (ffn_rows // 2 + 15) // 16 * 16
    halves = [(0, top), (top, ffn_rows - top)]
    if kind == "qkv":
        return [(k * head_rows, k * head_rows, k * merge * head_rows, head_rows, head_rows) for k in range(3)]
    if kind == "o":
        return [(0, 0, 0, head_rows, head_rows)]
    shift = ffn_rows if kind == "up" else 0
    return [(shift + off, off, off, ffn_rows, count) for off, count in halves]


class SumOverTg:
    def __init__(self, place, part, slots, full, sems):
        self.place, self.part, self.slots, self.full = place, part, slots, full
        self.count = slots.shape[1]
        self.send, self.recv = sems

    def scatter_copy(self, step):
        peer = self.place.tg_at(step)
        return pltpu.make_async_remote_copy(
            src_ref=rows(self.part, peer * self.count, self.count), dst_ref=self.slots.at[step - 1],
            send_sem=self.send.at[0, step - 1], recv_sem=self.recv.at[0, step - 1],
            device_id={"tg": peer}, device_id_type=MESH)

    def spread_copy(self, step):
        own = rows(self.full, self.place.tg * self.count, self.count)
        return pltpu.make_async_remote_copy(
            src_ref=own, dst_ref=own,
            send_sem=self.send.at[1, step - 1], recv_sem=self.recv.at[1, step - 1],
            device_id={"tg": self.place.tg_at(step)}, device_id_type=MESH)

    def spread_wait(self, step):
        peer = self.place.tg_at(self.place.tg_size - step)
        block = rows(self.full, peer * self.count, self.count)
        pltpu.make_async_remote_copy(
            src_ref=block, dst_ref=block,
            send_sem=self.send.at[1, step - 1], recv_sem=self.recv.at[1, step - 1],
            device_id={"tg": peer}, device_id_type=MESH).wait_recv()

    def steps(self):
        return range(1, self.place.tg_size)

    def far_first(self):
        return (2, 3, 1) if self.place.tg_size == 4 else self.steps()

    def scatter_start(self):
        for step in self.far_first():
            self.scatter_copy(step).start()

    def total(self):
        for step in self.steps():
            self.scatter_copy(step).wait_recv()
        out = self.part[pl.ds(pl.multiple_of(self.place.tg * self.count, self.count), self.count), :]
        for step in self.steps():
            out = out + self.slots[step - 1]
        return out

    def spread_start(self, block):
        self.full[pl.ds(pl.multiple_of(self.place.tg * self.count, self.count), self.count), :] = block
        for step in self.steps():
            self.scatter_copy(step).wait_send()
        for step in self.far_first():
            self.spread_copy(step).start()

    def spread_finish(self):
        for step in self.steps():
            self.spread_wait(step)
        for step in self.steps():
            self.spread_copy(step).wait_send()


def dot_nt(lhs, rhs):
    return lax.dot_general(lhs, rhs, (((1,), (1,)), ((), ())), preferred_element_type=F32)


def dot_nn(lhs, rhs):
    return jnp.dot(lhs, rhs, preferred_element_type=F32)


BOTH2, HALVES = ("both", "both"), ("owner", "other")


def first_kernel(tg_size, sizes, layers, hidden, lens, attn_gain, mlp_gain, w_qkv, w_o, w_gu, k_cache, v_cache,
                 normed, gains, cos_t, sin_t, qkv0, o0, k_next, v_next, gate_held,
                 hidden_buf, own_gain, far_gain, load_sem, gain_send, gain_recv, *sems):
    place = Place(tg_size)
    make = Maker(place, sems, sizes)
    units = make.gather("qkv", 0, w_qkv, qkv0, ("both",) * 3) + make.gather("o", 0, w_o, o0, ("both",))
    gate_piece = make.cross("gate", 0, w_gu, gate_held) + make.cross("gate", 1, w_gu, gate_held)
    loads = [pltpu.make_async_copy(src, dst, load_sem.at[k]) for k, (src, dst) in enumerate([
        (hidden, hidden_buf), (attn_gain, own_gain.at[0]), (mlp_gain, own_gain.at[1]),
        (k_cache.at[0], k_next), (v_cache.at[0], v_next)])]
    for copy in loads[:3]:
        copy.start()
    place.barrier(False)
    each(units, "start")
    for copy in loads[3:]:
        copy.start()
    for copy in loads[1:3]:
        copy.wait()
    gain_copies = [
        pltpu.make_async_remote_copy(
            src_ref=own_gain.at[k], dst_ref=far_gain.at[k], send_sem=gain_send.at[k], recv_sem=gain_recv.at[k],
            device_id={"pp": place.stage}, device_id_type=MESH) for k in range(2)]
    for copy in gain_copies:
        copy.start()
    each(gate_piece, "start")
    half = cos_t.shape[0]
    power = lax.broadcasted_iota(jnp.int32, cos_t.shape, 0).astype(F32) * (-math.log(ROPE_THETA) / half)
    angle = jnp.exp(power) * lens[...].astype(F32)
    cos_t[...] = jnp.cos(angle)
    sin_t[...] = jnp.sin(angle)
    each(units[:1], "send")
    for copy in gain_copies:
        copy.wait()
    loads[0].wait()
    first = place.pp == 0
    table = []
    for k in range(2):
        own_row, far_row = own_gain[k].astype(F32), far_gain[k].astype(F32)
        table.append(jnp.where(first, own_row, far_row))
        table.append(jnp.where(first, far_row, own_row))
    for k, row in enumerate(table):
        gains[pl.ds(k, 1), :] = row
    normed[...] = norm_rows(hidden_buf[...].astype(F32), table[0])
    each(units[1:2], "send")
    each(units[:1], "forward")
    each(units[2:3], "send")
    each(units[1:2], "forward")
    each(units[3:], "send")
    each(units[2:], "forward")
    each(units, "arrive")
    each(units, "finish")
    for copy in loads[3:]:
        copy.wait()
    each(gate_piece, "finish")


def attend_kernel(layer, head_dim, rest_in, lens, normed, w_qkv, cos_t, sin_t, k_in, v_in, *rest):
    rest = rest[rest_in:] if not layer else rest
    if layer:
        gate, up = rest[:2]
        rest = rest[2 + rest_in:]
        k_out, v_out, gen_qkv, gen_gu, attn_out = rest[:5]
        rest = rest[5:]
    else:
        k_out, v_out, gen_qkv, attn_out = rest[:4]
        rest = rest[4:]
    k_new, v_new, q_scr, k_scr, v_scr, kv_sem, gen_sem = rest
    gens = [pltpu.make_async_copy(w_qkv, gen_qkv.at[layer], gen_sem.at[0])]
    if layer:
        ffn = gate.shape[0]
        gens += [pltpu.make_async_copy(gate, gen_gu.at[0, pl.ds(0, ffn)], gen_sem.at[1]),
                 pltpu.make_async_copy(up, gen_gu.at[0, pl.ds(ffn, ffn)], gen_sem.at[2])]
    for copy in gens:
        copy.start()
    batch = normed.shape[0]
    width = q_scr.shape[1]
    heads = width // head_dim
    half = head_dim // 2
    cache_len = k_in.shape[2]
    proj = dot_nt(w_qkv[...], normed[...])
    cos_v, sin_v = cos_t[...], sin_t[...]

    def rope(block):
        pieces = []
        for head in range(heads):
            first = block[head * head_dim:head * head_dim + half]
            second = block[head * head_dim + half:(head + 1) * head_dim]
            pieces += [first * cos_v - second * sin_v, second * cos_v + first * sin_v]
        return jnp.concatenate(pieces, axis=0).astype(BF16).astype(F32)

    q_scr[...] = jnp.transpose(rope(proj[:width])) * (head_dim ** -0.5)
    pad = jnp.zeros((width, cache_len - batch), F32)
    k_scr[...] = jnp.concatenate([rope(proj[width:2 * width]), pad], axis=1)
    v_scr[...] = jnp.concatenate([proj[2 * width:].astype(BF16).astype(F32), pad], axis=1)
    lane = lax.broadcasted_iota(jnp.int32, (width, cache_len), 1)
    own_head = (lax.broadcasted_iota(jnp.int32, (HEAD_ROWS, width), 1) // head_dim
                == lax.broadcasted_iota(jnp.int32, (HEAD_ROWS, width), 0))
    lane_row = lax.broadcasted_iota(jnp.int32, (HEAD_ROWS, cache_len), 1)

    def copy_out(k, i):
        block = pl.ds(i * SEQ_TILE, SEQ_TILE)
        new, out = [(k_new, k_out), (v_new, v_out)][k]
        return pltpu.make_async_copy(new.at[block], out.at[layer, block], kv_sem.at[k, i])

    def placed(length, seq, cols, old):
        moved = pltpu.roll(cols, lax.rem(length - seq + cache_len, cache_len), 1).astype(BF16)
        return jnp.where(lane == length, moved, old)

    def step(i, carry):
        seq0 = i * SEQ_TILE
        k_cols, v_cols = k_scr[...], v_scr[...]
        scores = []
        for j in range(SEQ_TILE):
            length = lens[seq0 + j]
            k_val = placed(length, seq0 + j, k_cols, k_in[seq0 + j])
            k_new[seq0 + j] = k_val
            q_block = jnp.where(own_head, q_scr[pl.ds(seq0 + j, 1), :], 0.0).astype(BF16)
            scores.append(jnp.where(lane_row <= length, dot_nn(q_block, k_val), MASK_FILL))
        copy_out(0, i).start()
        score = jnp.concatenate(scores, axis=0)
        expo = jnp.exp(score - jnp.max(score, axis=-1, keepdims=True))
        probs = (expo / jnp.sum(expo, axis=-1, keepdims=True)).astype(BF16)
        outs = []
        for j in range(SEQ_TILE):
            v_val = placed(lens[seq0 + j], seq0 + j, v_cols, v_in[seq0 + j])
            v_new[seq0 + j] = v_val
            mixed = dot_nt(probs[j * HEAD_ROWS:(j + 1) * HEAD_ROWS], v_val)
            outs.append(jnp.sum(jnp.where(own_head, mixed, 0.0), axis=0, keepdims=True))
        copy_out(1, i).start()
        attn_out[pl.ds(pl.multiple_of(seq0, SEQ_TILE), SEQ_TILE), :] = jnp.concatenate(outs, axis=0).astype(BF16)
        return carry

    steps = batch // SEQ_TILE
    lax.fori_loop(0, steps, step, 0)
    for i in range(steps):
        copy_out(0, i).wait()
        copy_out(1, i).wait()
    for copy in gens:
        copy.wait()


def attend(layer, lens, normed, w_qkv, cos_t, sin_t, k_now, v_now, head_dim, layers, extra=(), prior=()):
    batch, width, cache_len = k_now.shape
    sds = jax.ShapeDtypeStruct
    flat = sds((layers,) + k_now.shape, BF16)
    gen = [sds((layers,) + w_qkv.shape, BF16)]
    if layer:
        gen.append(sds((layers, 2 * extra[0].shape[0], extra[0].shape[1]), BF16))
    return pl.pallas_call(
        functools.partial(attend_kernel, layer, head_dim, len(prior)),
        in_specs=[SMEM] + [VMEM] * (6 + len(extra)) + [HBM] * len(prior),
        out_specs=[HBM, HBM] + [HBM] * len(gen) + [VMEM],
        out_shape=[flat, flat] + gen + [sds((batch, width), BF16)],
        scratch_shapes=[pltpu.VMEM(k_now.shape, BF16)] * 2 + [
            pltpu.VMEM((batch, width), F32), pltpu.VMEM((width, cache_len), F32),
            pltpu.VMEM((width, cache_len), F32), pltpu.SemaphoreType.DMA((2, batch // SEQ_TILE)),
            pltpu.SemaphoreType.DMA((3,))],
        input_output_aliases={7 + len(extra) + k: k for k in range(len(prior))},
        compiler_params=pltpu.CompilerParams(vmem_limit_bytes=32 * 1024 * 1024),
        name=f"attend_{layer}",
    )(lens, normed, w_qkv, cos_t, sin_t, k_now, v_now, *extra, *prior)


def first_layer_kernel(tg_size, sizes, attn, hidden, gains, o0, gate_held, w_qkv, w_o, w_gu, w_dn, k_cache, v_cache,
                       normed, h_out, gate_buf, up_buf, qkv1, o1, k_next, v_next, up_held, dn_held,
                       dn_buf, part, slots, mid, h_own, load_sem, sum_send, sum_recv, *sems):
    place = Place(tg_size)
    make = Maker(place, sems, sizes)
    gate_u = make.gather("gate", 0, w_gu, gate_buf, BOTH2, gate_held)
    up_u = make.gather("up", 0, w_gu, up_buf, BOTH2)
    dn_u = make.gather("dn", 0, w_dn, dn_buf, ("both", "owner"))
    next_u = make.gather("qkv", 1, w_qkv, qkv1, ("both",) * 3) + make.gather("o", 1, w_o, o1, ("both",))
    crossing = make.cross("up", 1, w_gu, up_held) + make.cross("dn", 1, w_dn, dn_held)
    every = gate_u + up_u + dn_u + next_u
    sum_o = SumOverTg(place, part.at[0], slots.at[0], mid, (sum_send.at[0], sum_recv.at[0]))
    sum_d = SumOverTg(place, part.at[1], slots.at[1], normed, (sum_send.at[1], sum_recv.at[1]))
    count = slots.shape[2]
    loads = [pltpu.make_async_copy(src, dst, load_sem.at[k]) for k, (src, dst) in enumerate([
        (rows(hidden, place.tg * count, count), h_own), (k_cache.at[1], k_next), (v_cache.at[1], v_next)])]

    loads[0].start()
    place.barrier(True)
    each(every, "start")
    part[0] = dot_nn(attn[...], o0[...])
    sum_o.scatter_start()
    each(crossing, "start")
    each(gate_u, "send")
    for copy in loads[1:]:
        copy.start()
    gate_u[0].forward()
    up_u[0].send()
    gate_u[1].forward()
    loads[0].wait()
    h_mid = (h_own[...].astype(F32) + sum_o.total()).astype(BF16).astype(F32)
    sum_o.spread_start(norm_rows(h_mid, gains[2:3, :]))
    up_u[1].send()
    up_u[0].forward()
    dn_u[0].send()
    sum_o.spread_finish()
    each(gate_u, "arrive")
    act_in = mid[...]
    gate = jax.nn.silu(dot_nt(act_in, gate_buf[...]))
    up_u[1].forward()
    dn_u[1].send()
    each(next_u[:3], "send")
    each(up_u, "arrive")
    act = (gate * dot_nt(act_in, up_buf[...])).astype(BF16)
    each(next_u[3:], "send")
    each(dn_u, "forward")
    each(dn_u, "arrive")
    part[1] = dot_nn(act, dn_buf[...])
    sum_d.scatter_start()
    each(next_u[:2], "forward")
    h_new = (h_mid + sum_d.total()).astype(BF16)
    h_out[...] = h_new
    sum_d.spread_start(norm_rows(h_new.astype(F32), gains[1:2, :]))
    each(next_u[2:], "forward")
    sum_d.spread_finish()
    each(next_u, "arrive")
    each(every, "finish")
    each(crossing, "finish")
    for copy in loads[1:]:
        copy.wait()


def last_layer_kernel(tg_size, sizes, attn, h_in, gains, o1, gate_held, up_held, dn_held, w_gu, w_dn,
                      hidden_out, gate_buf, up_buf, dn_buf, part, slots, mid, sum_send, sum_recv, *sems):
    place = Place(tg_size)
    make = Maker(place, sems, sizes)
    gate_u = make.gather("gate", 1, w_gu, gate_buf, HALVES, gate_held)
    up_u = make.gather("up", 1, w_gu, up_buf, HALVES, up_held)
    dn_u = make.gather("dn", 1, w_dn, dn_buf, HALVES, dn_held)
    every = gate_u + up_u + dn_u
    sum_o = SumOverTg(place, part.at[0], slots.at[0], mid, (sum_send.at[0], sum_recv.at[0]))
    sum_d = SumOverTg(place, part.at[1], slots.at[1], hidden_out, (sum_send.at[1], sum_recv.at[1]))

    place.barrier(True)
    each(every, "start")
    part[0] = dot_nn(attn[...], o1[...])
    sum_o.scatter_start()
    each(every, "send")
    each(gate_u, "forward")
    h_mid = (h_in[...].astype(F32) + sum_o.total()).astype(BF16).astype(F32)
    sum_o.spread_start(norm_rows(h_mid, gains[3:4, :]))
    each(up_u, "forward")
    sum_o.spread_finish()
    each(gate_u, "arrive")
    act_in = mid[...]
    gate = jax.nn.silu(dot_nt(act_in, gate_buf[...]))
    each(dn_u, "forward")
    each(up_u, "arrive")
    act = (gate * dot_nt(act_in, up_buf[...])).astype(BF16)
    each(dn_u, "arrive")
    part[1] = dot_nn(act, dn_buf[...])
    sum_d.scatter_start()
    h_new = (h_mid + sum_d.total()).astype(BF16)
    sum_d.spread_start(h_new)
    each(every, "finish")
    sum_d.spread_finish()


def store_kernel(layer, gate, up, prior, gen_gu, sem):
    ffn = gate.shape[0]
    copies = [pltpu.make_async_copy(src, gen_gu.at[layer, pl.ds(k * ffn, ffn)], sem.at[k])
              for k, src in enumerate([gate, up])]
    for copy in copies:
        copy.start()
    for copy in copies:
        copy.wait()


def remote_params(collective_id):
    return pltpu.CompilerParams(collective_id=collective_id, has_side_effects=True,
                                vmem_limit_bytes=32 * 1024 * 1024)


def solution(mesh):
    merge = mesh.shape["grp"]
    tg_size = mesh.shape["tg"]
    cache_spec = P(None, ROW_AXES, None, "tg", None)
    in_specs = (P(ROW_AXES, None), P(ROW_AXES), cache_spec, cache_spec,
                P("pp", None), P("pp", TRAIN_AXES, None), P("pp", None, TRAIN_AXES),
                P("pp", None), P("pp", TRAIN_AXES, None), P("pp", None, TRAIN_AXES))
    out_specs = (P(ROW_AXES, None), cache_spec, cache_spec, P(None, "tg", None), P(None, "tg", None))

    def body(hidden_in, seq_lens, k_cache, v_cache, attn_gain, w_qkv, w_o, mlp_gain, w_gate_up, w_down):
        batch, dim = hidden_in.shape
        layers, _, cache_len, kv_loc, head_dim = k_cache.shape
        width = kv_loc * head_dim
        ffn_rows = w_gate_up.shape[1] // 2
        ffn = ffn_rows * merge
        sizes = (head_dim, ffn_rows, merge)
        quarter = batch // tg_size
        w_qkv, w_gate_up = w_qkv[0], w_gate_up[0]
        w_o_t, w_down_t = jnp.transpose(w_o[0]), jnp.transpose(w_down[0])
        flat = lambda cache: jnp.transpose(cache, (0, 1, 3, 4, 2)).reshape(layers, batch, width, cache_len)
        k_flat, v_flat = flat(k_cache), flat(v_cache)
        dma = pltpu.SemaphoreType.DMA
        sds = jax.ShapeDtypeStruct
        layer_kv = sds((batch, width, cache_len), BF16)
        merged_qkv, merged_o, merged_ffn = (sds((3 * width, dim), BF16), sds((width, dim), BF16), sds((ffn, dim), BF16))
        act, held = sds((batch, dim), BF16), sds((ffn_rows, dim), BF16)
        rope = sds((head_dim // 2, batch), F32)
        sum_scratch = [pltpu.VMEM((2, batch, dim), F32), pltpu.VMEM((2, tg_size - 1, quarter, dim), F32),
                       pltpu.VMEM((batch, dim), BF16)]
        sum_sems = [dma((2, 2, tg_size - 1)), dma((2, 2, tg_size - 1))]

        normed, gains, cos_t, sin_t, qkv0, o0, k_now, v_now, gate_held = pl.pallas_call(
            functools.partial(first_kernel, tg_size, sizes, layers),
            in_specs=[HBM, VMEM] + [HBM] * 7, out_specs=[VMEM] * 8 + [HBM],
            out_shape=[act, sds((4, dim), F32), rope, rope, merged_qkv, merged_o, layer_kv, layer_kv, held],
            scratch_shapes=[pltpu.VMEM((batch, dim), BF16), pltpu.VMEM((2, 1, dim), BF16),
                            pltpu.VMEM((2, 1, dim), BF16), dma((5,)), dma((2,)), dma((2,))] + gather_sems(8),
            compiler_params=remote_params(1), name="first",
        )(hidden_in, seq_lens.reshape(1, batch), attn_gain, mlp_gain, w_qkv, w_o_t, w_gate_up, k_flat, v_flat)

        k_out, v_out, gen_qkv, attn = attend(0, seq_lens, normed, qkv0, cos_t, sin_t, k_now, v_now, head_dim, layers)

        normed, h_own, gate0, up0, qkv1, o1, k_now, v_now, up_held, dn_held = pl.pallas_call(
            functools.partial(first_layer_kernel, tg_size, sizes),
            in_specs=[VMEM, HBM, VMEM, VMEM] + [HBM] * 7,
            out_specs=[VMEM] * 8 + [HBM, HBM],
            out_shape=[act, sds((quarter, dim), BF16), merged_ffn, merged_ffn, merged_qkv, merged_o,
                       layer_kv, layer_kv, held, held],
            scratch_shapes=[pltpu.VMEM((ffn, dim), BF16)] + sum_scratch + [
                pltpu.VMEM((quarter, dim), BF16), dma((3,))] + sum_sems + gather_sems(14),
            compiler_params=remote_params(2), name="layer_0",
        )(attn, hidden_in, gains, o0, gate_held, w_qkv, w_o_t, w_gate_up, w_down_t, k_flat, v_flat)

        k_out, v_out, gen_qkv, gen_gate_up, attn = attend(
            1, seq_lens, normed, qkv1, cos_t, sin_t, k_now, v_now, head_dim, layers,
            (gate0, up0), (k_out, v_out, gen_qkv))

        hidden, gate1, up1 = pl.pallas_call(
            functools.partial(last_layer_kernel, tg_size, sizes),
            in_specs=[VMEM] * 4 + [HBM] * 5, out_specs=[VMEM] * 3,
            out_shape=[act, merged_ffn, merged_ffn],
            scratch_shapes=[pltpu.VMEM((ffn, dim), BF16)] + sum_scratch + sum_sems + gather_sems(6),
            compiler_params=remote_params(3), name="layer_1",
        )(attn, h_own, gains, o1, gate_held, up_held, dn_held, w_gate_up, w_down_t)

        gen_gate_up = pl.pallas_call(
            functools.partial(store_kernel, 1),
            in_specs=[VMEM, VMEM, HBM], out_specs=HBM, out_shape=sds(gen_gate_up.shape, BF16),
            scratch_shapes=[dma((2,))], input_output_aliases={2: 0}, name="store",
        )(gate1, up1, gen_gate_up)

        unflat = lambda cache: jnp.transpose(
            cache.reshape(layers, batch, kv_loc, head_dim, cache_len), (0, 1, 4, 2, 3))
        return hidden, unflat(k_out), unflat(v_out), gen_qkv, gen_gate_up

    return jax.shard_map(body, mesh=mesh, in_specs=in_specs, out_specs=out_specs, check_vma=False)
```

```python
import functools
import math

import jax
import jax.numpy as jnp
from jax import lax
from jax.experimental import pallas as pl
from jax.experimental.pallas import tpu as pltpu
from jax.sharding import PartitionSpec as P

ROPE_THETA = 500000.0
NORM_EPS = 1e-5
MASK_FILL = -1e30
ROW_AXES = ("pp", "grp")
TRAIN_AXES = ("tg", "grp")
BF16 = jnp.bfloat16
F32 = jnp.float32
MESH = pl.DeviceIdType.MESH
HBM = pl.BlockSpec(memory_space=pltpu.HBM)
SMEM = pl.BlockSpec(memory_space=pltpu.SMEM)
VMEM = pl.BlockSpec(memory_space=pltpu.VMEM)
SEQ_TILE = 16
HEAD_ROWS = 8


def norm_rows(hidden_f32, gain_row):
    inv_rms = lax.rsqrt(jnp.mean(hidden_f32 * hidden_f32, axis=-1, keepdims=True) + NORM_EPS)
    return (hidden_f32 * inv_rms * gain_row).astype(BF16)


def rows(ref, start, count):
    return ref.at[pl.ds(pl.multiple_of(start, 16), count), :]


class Place:
    def __init__(self, tg_size):
        self.tg_size = tg_size
        self.tg = lax.axis_index("tg")
        self.pp = lax.axis_index("pp")
        self.grp = lax.axis_index("grp")
        self.partner = self.grp + 1 - 2 * lax.rem(self.grp, 2)
        self.across = lax.rem(self.grp + 2, 4)
        self.diagonal = lax.rem(self.partner + 2, 4)
        self.stage = 1 - self.pp

    def tg_at(self, step):
        return lax.rem(self.tg + step, self.tg_size)

    def barrier(self, with_tg):
        sem = pltpu.get_barrier_semaphore()
        targets = [{"grp": self.partner}, {"grp": self.across}, {"pp": self.stage}]
        if with_tg:
            targets += [{"tg": self.tg_at(step)} for step in range(1, self.tg_size)]
        for target in targets:
            pl.semaphore_signal(sem, inc=1, device_id=target, device_id_type=MESH)
        pl.semaphore_wait(sem, len(targets))


def gather_sems(count):
    dma = pltpu.SemaphoreType.DMA
    return [dma((count,)), dma((count, 2)), dma((count, 2)), dma((count, 2)), dma((count, 2, 2))]


class Cross:
    def __init__(self, place, sems, index, layer, own, held):
        self.place, self.layer = place, layer
        self.copy = lambda: pltpu.make_async_remote_copy(
            src_ref=own, dst_ref=held, send_sem=sems[1].at[index, 0], recv_sem=sems[1].at[index, 1],
            device_id={"pp": place.stage}, device_id_type=MESH)

    def start(self):
        @pl.when(self.place.pp == self.layer)
        def _():
            self.copy().start()

    def finish(self):
        @pl.when(self.place.pp == self.layer)
        def _():
            self.copy().wait_send()

        @pl.when(self.place.pp != self.layer)
        def _():
            self.copy().wait_recv()


class Gather:
    def __init__(self, place, sems, index, layer, own, held, buf, base, stride, count, route):
        self.place, self.layer, self.own, self.held, self.buf = place, layer, own, held, buf
        self.base, self.stride, self.count, self.route = base, stride, count, route
        local, ysem, zsem, xsem, psem = sems
        self.local = local.at[index]
        self.ysem = (ysem.at[index, 0], ysem.at[index, 1])
        self.zsem = (zsem.at[index, 0], zsem.at[index, 1])
        self.xsem = (xsem.at[index, 0], xsem.at[index, 1])
        self.psem = [(psem.at[index, k, 0], psem.at[index, k, 1]) for k in range(2)]

    def on(self, owner, body):
        pl.when(self.place.pp == self.layer if owner else self.place.pp != self.layer)(body)

    def at(self, grp):
        return rows(self.buf, self.base + grp * self.stride, self.count)

    def remote(self, src, grp, sems, target):
        return pltpu.make_async_remote_copy(
            src_ref=src, dst_ref=self.at(grp), send_sem=sems[0], recv_sem=sems[1],
            device_id=target, device_id_type=MESH)

    def local_copy(self, src):
        return pltpu.make_async_copy(src, self.at(self.place.grp), self.local)

    def y_copy(self):
        return self.remote(self.own, self.place.grp, self.ysem, {"pp": self.place.stage})

    def z_copy(self):
        grp = self.place.across
        return self.remote(self.at(grp), grp, self.zsem, {"pp": self.place.stage})

    def x_copy(self, grp):
        return self.remote(self.at(grp), grp, self.xsem, {"grp": self.place.across})

    def p_copy(self, grp, which):
        return self.remote(self.at(grp), grp, self.psem[which], {"grp": self.place.partner})

    def start(self):
        def owner():
            if self.held is None:
                self.y_copy().start()
            self.local_copy(self.own).start()

        self.on(True, owner)
        if self.held is not None:
            self.on(False, lambda: self.local_copy(self.held).start())

    def send(self):
        self.on(True, lambda: self.local_copy(self.own).wait())
        if self.held is None:
            self.on(False, lambda: self.y_copy().wait_recv())
        else:
            self.on(False, lambda: self.local_copy(self.held).wait())
        grp = self.place.grp
        if self.route == "both":
            self.x_copy(grp).start()
        else:
            self.on(self.route == "owner", lambda: self.x_copy(grp).start())
        self.p_copy(grp, 0).start()

    def relay(self):
        grp = self.place.across

        def pass_on():
            self.x_copy(grp).wait_recv()
            if self.route != "both":
                self.z_copy().start()
            self.p_copy(grp, 1).start()

        if self.route == "both":
            pass_on()
        else:
            self.on(self.route == "owner", pass_on)

    def receive(self):
        def take():
            self.z_copy().wait_recv()
            self.p_copy(self.place.across, 1).start()

        if self.route != "both":
            self.on(self.route != "owner", take)

    def arrive(self):
        self.p_copy(self.place.partner, 0).wait_recv()
        self.p_copy(self.place.diagonal, 1).wait_recv()

    def finish(self):
        if self.held is None:
            self.on(True, lambda: self.y_copy().wait_send())
        grp = self.place.grp
        if self.route == "both":
            self.x_copy(grp).wait_send()
        else:
            def relayed():
                self.x_copy(grp).wait_send()
                self.z_copy().wait_send()

            self.on(self.route == "owner", relayed)
        self.p_copy(grp, 0).wait_send()
        self.p_copy(self.place.across, 1).wait_send()


class Maker:
    def __init__(self, place, sems, sizes):
        self.place, self.sems, self.sizes, self.index = place, sems, sizes, 0

    def gather(self, kind, layer, src_ref, buf, routes, held=None):
        out = []
        for k, (src, hold, base, stride, count) in enumerate(row_blocks(kind, self.sizes)):
            route = routes[k % len(routes)]
            out.append(Gather(self.place, self.sems, self.index, layer, src_ref.at[pl.ds(src, count), :],
                              None if held is None else held.at[pl.ds(hold, count), :],
                              buf, base, stride, count, route))
            self.index += 1
        return out

    def cross(self, kind, layer, src_ref, held):
        count = self.sizes[1]
        src = count if kind == "up" else 0
        piece = Cross(self.place, self.sems, self.index, layer, src_ref.at[pl.ds(src, count), :], held)
        self.index += 1
        return [piece]


def each(units, what):
    for unit in units:
        getattr(unit, what)()


class Flow:
    def __init__(self, units, lag):
        self.events, self.done = [], 0
        for k in range(len(units) + lag):
            if k < len(units):
                self.events.append((units[k], "send"))
            if k >= lag:
                self.events.append((units[k - lag], "relay"))

    def through(self, unit, what):
        last = self.events.index((unit, what))
        while self.done <= last:
            piece, step = self.events[self.done]
            getattr(piece, step)()
            self.done += 1


def row_pieces(count, parts):
    size = (-(-count // parts) + 15) // 16 * 16
    return [(off, min(size, count - off)) for off in range(0, count, size)]


def row_blocks(kind, sizes):
    head_rows, ffn_rows, merge = sizes
    if kind in ("qkv", "o"):
        return [(k * head_rows + off, k * head_rows + off, k * merge * head_rows + off, head_rows, count)
                for k in range(3 if kind == "qkv" else 1) for off, count in row_pieces(head_rows, 2)]
    shift = ffn_rows if kind == "up" else 0
    return [(shift + off, off, off, ffn_rows, count) for off, count in row_pieces(ffn_rows, 4)]


class SumOverTg:
    def __init__(self, place, part, slots, full, sems):
        self.place, self.part, self.slots, self.full = place, part, slots, full
        self.count = slots.shape[1]
        self.send, self.recv = sems

    def scatter_copy(self, step):
        peer = self.place.tg_at(step)
        return pltpu.make_async_remote_copy(
            src_ref=rows(self.part, peer * self.count, self.count), dst_ref=self.slots.at[step - 1],
            send_sem=self.send.at[0, step - 1], recv_sem=self.recv.at[0, step - 1],
            device_id={"tg": peer}, device_id_type=MESH)

    def spread_copy(self, step):
        own = rows(self.full, self.place.tg * self.count, self.count)
        return pltpu.make_async_remote_copy(
            src_ref=own, dst_ref=own,
            send_sem=self.send.at[1, step - 1], recv_sem=self.recv.at[1, step - 1],
            device_id={"tg": self.place.tg_at(step)}, device_id_type=MESH)

    def spread_wait(self, step):
        peer = self.place.tg_at(self.place.tg_size - step)
        block = rows(self.full, peer * self.count, self.count)
        pltpu.make_async_remote_copy(
            src_ref=block, dst_ref=block,
            send_sem=self.send.at[1, step - 1], recv_sem=self.recv.at[1, step - 1],
            device_id={"tg": peer}, device_id_type=MESH).wait_recv()

    def steps(self):
        return range(1, self.place.tg_size)

    def far_first(self):
        return self.steps()

    def scatter_start(self):
        for step in self.far_first():
            self.scatter_copy(step).start()

    def total(self):
        for step in self.steps():
            self.scatter_copy(step).wait_recv()
        out = self.part[pl.ds(pl.multiple_of(self.place.tg * self.count, self.count), self.count), :]
        for step in self.steps():
            out = out + self.slots[step - 1]
        return out

    def spread_start(self, block):
        self.full[pl.ds(pl.multiple_of(self.place.tg * self.count, self.count), self.count), :] = block
        for step in self.steps():
            self.scatter_copy(step).wait_send()
        for step in self.far_first():
            self.spread_copy(step).start()

    def spread_finish(self):
        for step in self.steps():
            self.spread_wait(step)
        for step in self.steps():
            self.spread_copy(step).wait_send()


def dot_nt(lhs, rhs):
    return lax.dot_general(lhs, rhs, (((1,), (1,)), ((), ())), preferred_element_type=F32)


def dot_nn(lhs, rhs):
    return jnp.dot(lhs, rhs, preferred_element_type=F32)


BOTH, HALVES = ("both",), ("owner", "other")


def project(w_qkv, normed, cos_v, sin_v, head_dim, q_scr, k_scr, v_scr):
    batch, width = q_scr.shape
    half = head_dim // 2
    proj = dot_nt(w_qkv, normed)

    def rope(block):
        pieces = []
        for row in range(0, width, head_dim):
            first, second = block[row:row + half], block[row + half:row + head_dim]
            pieces += [first * cos_v - second * sin_v, second * cos_v + first * sin_v]
        return jnp.concatenate(pieces, axis=0).astype(BF16).astype(F32)

    q_scr[...] = jnp.transpose(rope(proj[:width])) * (head_dim ** -0.5)
    pad = jnp.zeros((width, k_scr.shape[1] - batch), F32)
    k_scr[...] = jnp.concatenate([rope(proj[width:2 * width]), pad], axis=1)
    v_scr[...] = jnp.concatenate([proj[2 * width:].astype(BF16).astype(F32), pad], axis=1)


def attend_tile(seq0, head_dim, lens, place_k, place_v, q_scr, k_in, v_in, k_new, v_new, after_keys):
    width, cache_len = k_in.shape[1:]
    own_head = (lax.broadcasted_iota(jnp.int32, (HEAD_ROWS, width), 1) // head_dim
                == lax.broadcasted_iota(jnp.int32, (HEAD_ROWS, width), 0))
    lane_row = lax.broadcasted_iota(jnp.int32, (HEAD_ROWS, cache_len), 1)
    scores = []
    for j in range(SEQ_TILE):
        length = lens[seq0 + j]
        k_val = place_k(length, j, k_in[seq0 + j])
        k_new[seq0 + j] = k_val
        q_block = jnp.where(own_head, q_scr[pl.ds(seq0 + j, 1), :], 0.0).astype(BF16)
        scores.append(jnp.where(lane_row <= length, dot_nn(q_block, k_val), MASK_FILL))
    after_keys()
    score = jnp.concatenate(scores, axis=0)
    expo = jnp.exp(score - jnp.max(score, axis=-1, keepdims=True))
    probs = (expo / jnp.sum(expo, axis=-1, keepdims=True)).astype(BF16)
    outs = []
    for j in range(SEQ_TILE):
        v_val = place_v(lens[seq0 + j], j, v_in[seq0 + j])
        v_new[seq0 + j] = v_val
        mixed = dot_nt(probs[j * HEAD_ROWS:(j + 1) * HEAD_ROWS], v_val)
        outs.append(jnp.sum(jnp.where(own_head, mixed, 0.0), axis=0, keepdims=True))
    return jnp.concatenate(outs, axis=0).astype(BF16)


def opening_kernel(tg_size, sizes, lens, lens_row, hidden, attn_gain, mlp_gain, w_qkv, w_o, w_gu, w_dn, k_cache, v_cache,
                   normed, h_out, gains, cos_t, sin_t, gate_buf, up_buf, qkv0, qkv1, o1, k_first, v_first,
                   k_next, v_next, gate_held, up_held, dn_held,
                   o_buf, dn_buf, part, slots, mid, hidden_buf, first_norm, attn, q_scr, k_scr, v_scr, own_gain, far_gain,
                   load_sem, gain_send, gain_recv, sum_send, sum_recv, *sems):
    head_dim = sizes[0]
    place = Place(tg_size)
    make = Maker(place, sems, sizes)
    qkv_u = make.gather("qkv", 0, w_qkv, qkv0, BOTH)
    o_u = make.gather("o", 0, w_o, o_buf, BOTH)
    gate_u = make.gather("gate", 0, w_gu, gate_buf, BOTH)
    up_u = make.gather("up", 0, w_gu, up_buf, BOTH)
    dn_u = make.gather("dn", 0, w_dn, dn_buf, BOTH)
    now_u = qkv_u + o_u + gate_u + up_u + dn_u
    next_u = make.gather("qkv", 1, w_qkv, qkv1, BOTH) + make.gather("o", 1, w_o, o1, BOTH)
    crossing = (make.cross("gate", 1, w_gu, gate_held) + make.cross("up", 1, w_gu, up_held)
                + make.cross("dn", 1, w_dn, dn_held))
    flow = Flow(now_u, 2)
    sum_o = SumOverTg(place, part.at[0], slots.at[0], mid, (sum_send.at[0], sum_recv.at[0]))
    sum_d = SumOverTg(place, part.at[1], slots.at[1], normed, (sum_send.at[1], sum_recv.at[1]))
    count = slots.shape[2]
    loads = [pltpu.make_async_copy(src, dst, load_sem.at[k]) for k, (src, dst) in enumerate([
        (hidden, hidden_buf), (attn_gain, own_gain.at[0]), (mlp_gain, own_gain.at[1]),
        (k_cache.at[0], k_first), (v_cache.at[0], v_first), (k_cache.at[1], k_next), (v_cache.at[1], v_next)])]

    for copy in loads[:3]:
        copy.start()
    place.barrier(True)
    each(qkv_u + o_u, "start")
    for copy in loads[1:3]:
        copy.wait()
    gain_copies = [
        pltpu.make_async_remote_copy(
            src_ref=own_gain.at[k], dst_ref=far_gain.at[k], send_sem=gain_send.at[k], recv_sem=gain_recv.at[k],
            device_id={"pp": place.stage}, device_id_type=MESH) for k in range(2)]
    for copy in gain_copies:
        copy.start()
    each(gate_u + up_u + dn_u + next_u, "start")
    each(crossing, "start")
    for copy in loads[3:5]:
        copy.start()
    half = cos_t.shape[0]
    power = lax.broadcasted_iota(jnp.int32, cos_t.shape, 0).astype(F32) * (-math.log(ROPE_THETA) / half)
    angle = jnp.exp(power) * lens_row[...].astype(F32)
    cos_t[...] = jnp.cos(angle)
    sin_t[...] = jnp.sin(angle)
    flow.through(qkv_u[1], "send")
    loads[0].wait()
    for copy in gain_copies:
        copy.wait()
    first = place.pp == 0
    table = []
    for k in range(2):
        own_row, far_row = own_gain[k].astype(F32), far_gain[k].astype(F32)
        table.append(jnp.where(first, own_row, far_row))
        table.append(jnp.where(first, far_row, own_row))
    for k, row in enumerate(table):
        gains[pl.ds(k, 1), :] = row
    first_norm[...] = norm_rows(hidden_buf[...].astype(F32), table[0])
    flow.through(qkv_u[-1], "relay")
    each(qkv_u, "arrive")
    project(qkv0[...], first_norm[...], cos_t[...], sin_t[...], head_dim, q_scr, k_scr, v_scr)
    for copy in loads[3:5]:
        copy.wait()

    lane = lax.broadcasted_iota(jnp.int32, k_first.shape[1:], 1)
    marks = [(o_u[-1], "relay"), (gate_u[0], "relay"), (gate_u[1], "relay"), (gate_u[3], "send")]
    for tile, mark in enumerate(marks):
        seq0 = tile * SEQ_TILE
        k_cols, v_cols = k_scr[...].astype(BF16), v_scr[...].astype(BF16)
        put_k = lambda length, j, old: jnp.where(lane == length, k_cols[:, seq0 + j:seq0 + j + 1], old)
        put_v = lambda length, j, old: jnp.where(lane == length, v_cols[:, seq0 + j:seq0 + j + 1], old)
        attn[pl.ds(seq0, SEQ_TILE), :] = attend_tile(
            seq0, head_dim, lens, put_k, put_v, q_scr, k_first, v_first, k_first, v_first, lambda: None)
        flow.through(*mark)

    for copy in loads[5:]:
        copy.start()
    each(o_u, "arrive")
    part[0] = dot_nn(attn[...], o_buf[...])
    sum_o.scatter_start()
    flow.through(up_u[1], "relay")
    own_rows = hidden_buf[pl.ds(pl.multiple_of(place.tg * count, count), count), :]
    h_mid = (own_rows.astype(F32) + sum_o.total()).astype(BF16).astype(F32)
    sum_o.spread_start(norm_rows(h_mid, gains[2:3, :]))
    flow.through(up_u[-1], "relay")
    each(gate_u, "arrive")
    sum_o.spread_finish()
    act_in = mid[...]
    gate = jax.nn.silu(dot_nt(act_in, gate_buf[...]))
    each(up_u, "arrive")
    act = (gate * dot_nt(act_in, up_buf[...])).astype(BF16)
    flow.through(dn_u[-1], "send")
    each(next_u, "send")
    flow.through(dn_u[-1], "relay")
    each(dn_u, "arrive")
    part[1] = dot_nn(act, dn_buf[...])
    sum_d.scatter_start()
    each(next_u[:4], "relay")
    h_new = (h_mid + sum_d.total()).astype(BF16)
    h_out[...] = h_new
    sum_d.spread_start(norm_rows(h_new.astype(F32), gains[1:2, :]))
    each(next_u[4:], "relay")
    each(now_u, "finish")
    each(crossing, "finish")
    sum_d.spread_finish()
    each(next_u, "arrive")
    each(next_u, "finish")
    for copy in loads[5:]:
        copy.wait()


def attend_kernel(head_dim, lens, normed, w_qkv, cos_t, sin_t, k_in, v_in, w_first, gate, up, k_first, v_first,
                  k_out, v_out, gen_qkv, gen_gu, attn_out, k_new, v_new, q_scr, k_scr, v_scr, kv_sem, gen_sem):
    ffn = gate.shape[0]
    gens = [pltpu.make_async_copy(src, dst, gen_sem.at[k]) for k, (src, dst) in enumerate([
        (k_first, k_out.at[0]), (v_first, v_out.at[0]), (w_first, gen_qkv.at[0]), (w_qkv, gen_qkv.at[1]),
        (gate, gen_gu.at[0, pl.ds(0, ffn)]), (up, gen_gu.at[0, pl.ds(ffn, ffn)])])]
    for copy in gens:
        copy.start()
    batch, width = q_scr.shape
    cache_len = k_in.shape[2]
    project(w_qkv[...], normed[...], cos_t[...], sin_t[...], head_dim, q_scr, k_scr, v_scr)
    lane = lax.broadcasted_iota(jnp.int32, (width, cache_len), 1)

    def copy_out(k, i):
        block = pl.ds(i * SEQ_TILE, SEQ_TILE)
        new, out = [(k_new, k_out), (v_new, v_out)][k]
        return pltpu.make_async_copy(new.at[block], out.at[1, block], kv_sem.at[k, i])

    def step(i, carry):
        seq0 = i * SEQ_TILE

        def placer(cols):
            def place(length, j, old):
                moved = pltpu.roll(cols, lax.rem(length - seq0 - j + cache_len, cache_len), 1).astype(BF16)
                return jnp.where(lane == length, moved, old)

            return place

        out = attend_tile(seq0, head_dim, lens, placer(k_scr[...]), placer(v_scr[...]), q_scr, k_in, v_in, k_new, v_new,
                          lambda: copy_out(0, i).start())
        copy_out(1, i).start()
        attn_out[pl.ds(pl.multiple_of(seq0, SEQ_TILE), SEQ_TILE), :] = out
        return carry

    steps = batch // SEQ_TILE
    lax.fori_loop(0, steps, step, 0)
    for i in range(steps):
        copy_out(0, i).wait()
        copy_out(1, i).wait()
    for copy in gens:
        copy.wait()


def last_layer_kernel(tg_size, sizes, attn, h_in, gains, o1, gate_held, up_held, dn_held, w_gu, w_dn,
                      hidden_out, gate_buf, up_buf, dn_buf, part, slots, mid, sum_send, sum_recv, *sems):
    place = Place(tg_size)
    make = Maker(place, sems, sizes)
    gate_u = make.gather("gate", 1, w_gu, gate_buf, HALVES, gate_held)
    up_u = make.gather("up", 1, w_gu, up_buf, HALVES, up_held)
    dn_u = make.gather("dn", 1, w_dn, dn_buf, HALVES, dn_held)
    every = gate_u + up_u + dn_u
    sum_o = SumOverTg(place, part.at[0], slots.at[0], mid, (sum_send.at[0], sum_recv.at[0]))
    sum_d = SumOverTg(place, part.at[1], slots.at[1], hidden_out, (sum_send.at[1], sum_recv.at[1]))

    place.barrier(True)
    each(every, "start")
    part[0] = dot_nn(attn[...], o1[...])
    sum_o.scatter_start()
    each(every, "send")
    each(gate_u, "relay")
    h_mid = (h_in[...].astype(F32) + sum_o.total()).astype(BF16).astype(F32)
    sum_o.spread_start(norm_rows(h_mid, gains[3:4, :]))
    each(gate_u, "receive")
    each(up_u, "relay")
    each(gate_u, "arrive")
    sum_o.spread_finish()
    act_in = mid[...]
    gate = jax.nn.silu(dot_nt(act_in, gate_buf[...]))
    each(dn_u, "relay")
    each(up_u, "receive")
    each(up_u, "arrive")
    act = (gate * dot_nt(act_in, up_buf[...])).astype(BF16)
    each(dn_u, "receive")
    each(dn_u, "arrive")
    part[1] = dot_nn(act, dn_buf[...])
    sum_d.scatter_start()
    each(every, "finish")
    h_new = (h_mid + sum_d.total()).astype(BF16)
    sum_d.spread_start(h_new)
    sum_d.spread_finish()


def store_kernel(layer, gate, up, prior, gen_gu, sem):
    ffn = gate.shape[0]
    copies = [pltpu.make_async_copy(src, gen_gu.at[layer, pl.ds(k * ffn, ffn)], sem.at[k])
              for k, src in enumerate([gate, up])]
    for copy in copies:
        copy.start()
    for copy in copies:
        copy.wait()


MIB = 1024 * 1024
OPENING_VMEM, ATTEND_VMEM, LAST_VMEM = 34 * MIB, 34 * MIB, 34 * MIB


def remote_params(collective_id, limit):
    return pltpu.CompilerParams(collective_id=collective_id, has_side_effects=True, vmem_limit_bytes=limit)


def solution(mesh):
    merge = mesh.shape["grp"]
    tg_size = mesh.shape["tg"]
    cache_spec = P(None, ROW_AXES, None, "tg", None)
    in_specs = (P(ROW_AXES, None), P(ROW_AXES), cache_spec, cache_spec,
                P("pp", None), P("pp", TRAIN_AXES, None), P("pp", None, TRAIN_AXES),
                P("pp", None), P("pp", TRAIN_AXES, None), P("pp", None, TRAIN_AXES))
    out_specs = (P(ROW_AXES, None), cache_spec, cache_spec, P(None, "tg", None), P(None, "tg", None))

    def body(hidden_in, seq_lens, k_cache, v_cache, attn_gain, w_qkv, w_o, mlp_gain, w_gate_up, w_down):
        batch, dim = hidden_in.shape
        layers, _, cache_len, kv_loc, head_dim = k_cache.shape
        width = kv_loc * head_dim
        ffn_rows = w_gate_up.shape[1] // 2
        ffn = ffn_rows * merge
        sizes = (head_dim, ffn_rows, merge)
        quarter = batch // tg_size
        w_qkv, w_gate_up = w_qkv[0], w_gate_up[0]
        w_o_t, w_down_t = jnp.transpose(w_o[0]), jnp.transpose(w_down[0])
        flat = lambda cache: jnp.transpose(cache, (0, 1, 3, 4, 2)).reshape(layers, batch, width, cache_len)
        k_flat, v_flat = flat(k_cache), flat(v_cache)
        dma = pltpu.SemaphoreType.DMA
        sds = jax.ShapeDtypeStruct
        layer_kv = sds((batch, width, cache_len), BF16)
        merged_qkv, merged_o, merged_ffn = (sds((3 * width, dim), BF16), sds((width, dim), BF16), sds((ffn, dim), BF16))
        act, held = sds((batch, dim), BF16), sds((ffn_rows, dim), BF16)
        rope = sds((head_dim // 2, batch), F32)
        sum_scratch = [pltpu.VMEM((2, batch, dim), F32), pltpu.VMEM((2, tg_size - 1, quarter, dim), F32),
                       pltpu.VMEM((batch, dim), BF16)]
        sum_sems = [dma((2, 2, tg_size - 1)), dma((2, 2, tg_size - 1))]

        projected = [pltpu.VMEM((batch, width), F32), pltpu.VMEM((width, cache_len), F32),
                     pltpu.VMEM((width, cache_len), F32)]
        on_chip = lambda like: pltpu.VMEM(like.shape, like.dtype)
        off_chip = lambda like: pltpu.HBM(like.shape, like.dtype)
        hbm = lambda *arrays: [pltpu.with_memory_space_constraint(arr, pltpu.HBM) for arr in arrays]
        vmem = lambda *arrays: [pltpu.with_memory_space_constraint(arr, pltpu.VMEM) for arr in arrays]
        shared = [act, sds((quarter, dim), BF16), sds((4, dim), F32), rope, rope, merged_ffn, merged_ffn,
                  merged_qkv, merged_qkv, merged_o, layer_kv, layer_kv, layer_kv, layer_kv]
        (normed, h_own, gains, cos_t, sin_t, gate0, up0, qkv0, qkv1, o1, k_first, v_first, k_next, v_next,
         gate_held, up_held, dn_held) = pl.pallas_call(
            functools.partial(opening_kernel, tg_size, sizes),
            in_specs=[SMEM, VMEM] + [HBM] * 9, out_specs=[VMEM] * 14 + [HBM] * 3,
            out_shape=[on_chip(x) for x in shared] + [off_chip(held)] * 3,
            scratch_shapes=[pltpu.VMEM((width, dim), BF16), pltpu.VMEM((ffn, dim), BF16)] + sum_scratch + [
                pltpu.VMEM((batch, dim), BF16), pltpu.VMEM((batch, dim), BF16), pltpu.VMEM((batch, width), BF16)]
            + projected + [pltpu.VMEM((2, 1, dim), BF16), pltpu.VMEM((2, 1, dim), BF16),
                           dma((7,)), dma((2,)), dma((2,))] + sum_sems + gather_sems(31),
            compiler_params=remote_params(1, OPENING_VMEM), name="opening",
        )(seq_lens, seq_lens.reshape(1, batch), *hbm(hidden_in, attn_gain, mlp_gain, w_qkv, w_o_t, w_gate_up, w_down_t,
                                                     k_flat, v_flat))

        cache_shape = off_chip(k_flat)
        k_out, v_out, gen_qkv, gen_gate_up, attn = pl.pallas_call(
            functools.partial(attend_kernel, head_dim),
            in_specs=[SMEM] + [VMEM] * 11, out_specs=[HBM] * 4 + [VMEM],
            out_shape=[cache_shape, cache_shape, pltpu.HBM((layers, 3 * width, dim), BF16),
                       pltpu.HBM((layers, 2 * ffn, dim), BF16), pltpu.VMEM((batch, width), BF16)],
            scratch_shapes=[pltpu.VMEM(layer_kv.shape, BF16)] * 2 + projected + [
                dma((2, batch // SEQ_TILE)), dma((6,))],
            compiler_params=pltpu.CompilerParams(vmem_limit_bytes=ATTEND_VMEM), name="attend",
        )(seq_lens, *vmem(normed, qkv1, cos_t, sin_t, k_next, v_next, qkv0, gate0, up0, k_first, v_first))

        hidden, gate1, up1 = pl.pallas_call(
            functools.partial(last_layer_kernel, tg_size, sizes),
            in_specs=[VMEM] * 4 + [HBM] * 5, out_specs=[VMEM] * 3,
            out_shape=[on_chip(act), on_chip(merged_ffn), on_chip(merged_ffn)],
            scratch_shapes=[pltpu.VMEM((ffn, dim), BF16)] + sum_scratch + sum_sems + gather_sems(12),
            compiler_params=remote_params(2, LAST_VMEM), name="layer_1",
        )(*vmem(attn, h_own, gains, o1), *hbm(gate_held, up_held, dn_held, w_gate_up, w_down_t))

        gen_gate_up = pl.pallas_call(
            functools.partial(store_kernel, 1),
            in_specs=[VMEM, VMEM, HBM], out_specs=HBM, out_shape=pltpu.HBM(gen_gate_up.shape, BF16),
            scratch_shapes=[dma((2,))], input_output_aliases={2: 0}, name="store",
        )(*vmem(gate1, up1), gen_gate_up)

        unflat = lambda cache: jnp.transpose(
            cache.reshape(layers, batch, kv_loc, head_dim, cache_len), (0, 1, 4, 2, 3))
        return hidden, unflat(k_out), unflat(v_out), gen_qkv, gen_gate_up

    return jax.shard_map(body, mesh=mesh, in_specs=in_specs, out_specs=out_specs, check_vma=False)
```

```python
import functools
import math

import jax
import jax.numpy as jnp
from jax import lax
from jax.experimental import pallas as pl
from jax.experimental.pallas import tpu as pltpu
from jax.sharding import PartitionSpec as P

ROPE_THETA = 500000.0
NORM_EPS = 1e-5
MASK_FILL = -1e30
ROW_AXES = ("pp", "grp")
TRAIN_AXES = ("tg", "grp")
BF16 = jnp.bfloat16
F32 = jnp.float32
MESH = pl.DeviceIdType.MESH
HBM = pl.BlockSpec(memory_space=pltpu.HBM)
SMEM = pl.BlockSpec(memory_space=pltpu.SMEM)
VMEM = pl.BlockSpec(memory_space=pltpu.VMEM)
SEQ_TILE = 16
HEAD_ROWS = 8


def norm_rows(hidden_f32, gain_row):
    inv_rms = lax.rsqrt(jnp.mean(hidden_f32 * hidden_f32, axis=-1, keepdims=True) + NORM_EPS)
    return (hidden_f32 * inv_rms * gain_row).astype(BF16)


def rows(ref, start, count):
    return ref.at[pl.ds(pl.multiple_of(start, 16), count), :]


class Place:
    def __init__(self, tg_size):
        self.tg_size = tg_size
        self.tg = lax.axis_index("tg")
        self.pp = lax.axis_index("pp")
        self.grp = lax.axis_index("grp")
        self.partner = self.grp + 1 - 2 * lax.rem(self.grp, 2)
        self.across = lax.rem(self.grp + 2, 4)
        self.diagonal = lax.rem(self.partner + 2, 4)
        self.stage = 1 - self.pp

    def tg_at(self, step):
        return lax.rem(self.tg + step, self.tg_size)

    def barrier(self, with_tg):
        sem = pltpu.get_barrier_semaphore()
        targets = [{"grp": self.partner}, {"grp": self.across}, {"pp": self.stage}]
        if with_tg:
            targets += [{"tg": self.tg_at(step)} for step in range(1, self.tg_size)]
        for target in targets:
            pl.semaphore_signal(sem, inc=1, device_id=target, device_id_type=MESH)
        pl.semaphore_wait(sem, len(targets))


def gather_sems(count):
    dma = pltpu.SemaphoreType.DMA
    return [dma((count,)), dma((count, 2)), dma((count, 2)), dma((count, 2)), dma((count, 2, 2))]


class Cross:
    def __init__(self, place, sems, index, layer, own, held):
        self.place, self.layer = place, layer
        self.copy = lambda: pltpu.make_async_remote_copy(
            src_ref=own, dst_ref=held, send_sem=sems[1].at[index, 0], recv_sem=sems[1].at[index, 1],
            device_id={"pp": place.stage}, device_id_type=MESH)

    def start(self):
        @pl.when(self.place.pp == self.layer)
        def _():
            self.copy().start()

    def finish(self):
        @pl.when(self.place.pp == self.layer)
        def _():
            self.copy().wait_send()

        @pl.when(self.place.pp != self.layer)
        def _():
            self.copy().wait_recv()


class Gather:
    def __init__(self, place, sems, index, layer, own, held, buf, base, stride, count, route):
        self.place, self.layer, self.own, self.held, self.buf = place, layer, own, held, buf
        self.base, self.stride, self.count, self.route = base, stride, count, route
        local, ysem, zsem, xsem, psem = sems
        self.local = local.at[index]
        self.ysem = (ysem.at[index, 0], ysem.at[index, 1])
        self.zsem = (zsem.at[index, 0], zsem.at[index, 1])
        self.xsem = (xsem.at[index, 0], xsem.at[index, 1])
        self.psem = [(psem.at[index, k, 0], psem.at[index, k, 1]) for k in range(2)]

    def on(self, owner, body):
        pl.when(self.place.pp == self.layer if owner else self.place.pp != self.layer)(body)

    def at(self, grp):
        return rows(self.buf, self.base + grp * self.stride, self.count)

    def remote(self, src, grp, sems, target):
        return pltpu.make_async_remote_copy(
            src_ref=src, dst_ref=self.at(grp), send_sem=sems[0], recv_sem=sems[1],
            device_id=target, device_id_type=MESH)

    def local_copy(self, src):
        return pltpu.make_async_copy(src, self.at(self.place.grp), self.local)

    def y_copy(self):
        return self.remote(self.own, self.place.grp, self.ysem, {"pp": self.place.stage})

    def z_copy(self):
        grp = self.place.across
        return self.remote(self.at(grp), grp, self.zsem, {"pp": self.place.stage})

    def x_copy(self, grp):
        return self.remote(self.at(grp), grp, self.xsem, {"grp": self.place.across})

    def p_copy(self, grp, which):
        return self.remote(self.at(grp), grp, self.psem[which], {"grp": self.place.partner})

    def start(self):
        def owner():
            if self.held is None:
                self.y_copy().start()
            self.local_copy(self.own).start()

        self.on(True, owner)
        if self.held is not None:
            self.on(False, lambda: self.local_copy(self.held).start())

    def send(self):
        self.on(True, lambda: self.local_copy(self.own).wait())
        if self.held is None:
            self.on(False, lambda: self.y_copy().wait_recv())
        else:
            self.on(False, lambda: self.local_copy(self.held).wait())
        grp = self.place.grp
        if self.route == "both":
            self.x_copy(grp).start()
        else:
            self.on(self.route == "owner", lambda: self.x_copy(grp).start())
        self.p_copy(grp, 0).start()

    def relay(self):
        grp = self.place.across

        def pass_on():
            self.x_copy(grp).wait_recv()
            if self.route != "both":
                self.z_copy().start()
            self.p_copy(grp, 1).start()

        if self.route == "both":
            pass_on()
        else:
            self.on(self.route == "owner", pass_on)

    def receive(self):
        def take():
            self.z_copy().wait_recv()
            self.p_copy(self.place.across, 1).start()

        if self.route != "both":
            self.on(self.route != "owner", take)

    def arrive(self):
        self.p_copy(self.place.partner, 0).wait_recv()
        self.p_copy(self.place.diagonal, 1).wait_recv()

    def finish(self):
        if self.held is None:
            self.on(True, lambda: self.y_copy().wait_send())
        grp = self.place.grp
        if self.route == "both":
            self.x_copy(grp).wait_send()
        else:
            def relayed():
                self.x_copy(grp).wait_send()
                self.z_copy().wait_send()

            self.on(self.route == "owner", relayed)
        self.p_copy(grp, 0).wait_send()
        self.p_copy(self.place.across, 1).wait_send()


class Maker:
    def __init__(self, place, sems, sizes):
        self.place, self.sems, self.sizes, self.index = place, sems, sizes, 0

    def gather(self, kind, layer, src_ref, buf, routes, held=None):
        out = []
        for k, (src, hold, base, stride, count) in enumerate(row_blocks(kind, self.sizes)):
            route = routes[k % len(routes)]
            out.append(Gather(self.place, self.sems, self.index, layer, src_ref.at[pl.ds(src, count), :],
                              None if held is None else held.at[pl.ds(hold, count), :],
                              buf, base, stride, count, route))
            self.index += 1
        return out

    def cross(self, kind, layer, src_ref, held):
        count = self.sizes[1]
        src = count if kind == "up" else 0
        piece = Cross(self.place, self.sems, self.index, layer, src_ref.at[pl.ds(src, count), :], held)
        self.index += 1
        return [piece]


def each(units, what):
    for unit in units:
        getattr(unit, what)()


class Flow:
    def __init__(self, units, lag):
        self.events, self.done = [], 0
        for k in range(len(units) + lag):
            if k < len(units):
                self.events.append((units[k], "send"))
            if k >= lag:
                self.events.append((units[k - lag], "relay"))

    def through(self, unit, what):
        last = self.events.index((unit, what))
        while self.done <= last:
            piece, step = self.events[self.done]
            getattr(piece, step)()
            self.done += 1


def row_pieces(count, parts):
    size = (-(-count // parts) + 15) // 16 * 16
    return [(off, min(size, count - off)) for off in range(0, count, size)]


def row_blocks(kind, sizes):
    head_rows, ffn_rows, merge = sizes
    if kind in ("qkv", "o"):
        return [(k * head_rows + off, k * head_rows + off, k * merge * head_rows + off, head_rows, count)
                for k in range(3 if kind == "qkv" else 1) for off, count in row_pieces(head_rows, 2)]
    shift = ffn_rows if kind == "up" else 0
    return [(shift + off, off, off, ffn_rows, count) for off, count in row_pieces(ffn_rows, 4)]


class SumOverTg:
    def __init__(self, place, part, slots, full, sems):
        self.place, self.part, self.slots, self.full = place, part, slots, full
        self.count = slots.shape[1]
        self.send, self.recv = sems

    def scatter_copy(self, step):
        peer = self.place.tg_at(step)
        return pltpu.make_async_remote_copy(
            src_ref=rows(self.part, peer * self.count, self.count), dst_ref=self.slots.at[step - 1],
            send_sem=self.send.at[0, step - 1], recv_sem=self.recv.at[0, step - 1],
            device_id={"tg": peer}, device_id_type=MESH)

    def spread_copy(self, step):
        own = rows(self.full, self.place.tg * self.count, self.count)
        return pltpu.make_async_remote_copy(
            src_ref=own, dst_ref=own,
            send_sem=self.send.at[1, step - 1], recv_sem=self.recv.at[1, step - 1],
            device_id={"tg": self.place.tg_at(step)}, device_id_type=MESH)

    def spread_wait(self, step):
        peer = self.place.tg_at(self.place.tg_size - step)
        block = rows(self.full, peer * self.count, self.count)
        pltpu.make_async_remote_copy(
            src_ref=block, dst_ref=block,
            send_sem=self.send.at[1, step - 1], recv_sem=self.recv.at[1, step - 1],
            device_id={"tg": peer}, device_id_type=MESH).wait_recv()

    def steps(self):
        return range(1, self.place.tg_size)

    def far_first(self):
        return self.steps()

    def scatter_start(self):
        for step in self.far_first():
            self.scatter_copy(step).start()

    def total(self):
        for step in self.steps():
            self.scatter_copy(step).wait_recv()
        out = self.part[pl.ds(pl.multiple_of(self.place.tg * self.count, self.count), self.count), :]
        for step in self.steps():
            out = out + self.slots[step - 1]
        return out

    def spread_start(self, block):
        self.full[pl.ds(pl.multiple_of(self.place.tg * self.count, self.count), self.count), :] = block
        for step in self.steps():
            self.scatter_copy(step).wait_send()
        for step in self.far_first():
            self.spread_copy(step).start()

    def spread_finish(self):
        for step in self.steps():
            self.spread_wait(step)
        for step in self.steps():
            self.spread_copy(step).wait_send()


def dot_nt(lhs, rhs):
    return lax.dot_general(lhs, rhs, (((1,), (1,)), ((), ())), preferred_element_type=F32)


def dot_nn(lhs, rhs):
    return jnp.dot(lhs, rhs, preferred_element_type=F32)


BOTH, HALVES = ("both",), ("owner", "other")


def project(w_qkv, normed, cos_v, sin_v, head_dim, q_scr, k_scr, v_scr):
    batch, width = q_scr.shape
    half = head_dim // 2
    proj = dot_nt(w_qkv, normed)

    def rope(block):
        pieces = []
        for row in range(0, width, head_dim):
            first, second = block[row:row + half], block[row + half:row + head_dim]
            pieces += [first * cos_v - second * sin_v, second * cos_v + first * sin_v]
        return jnp.concatenate(pieces, axis=0).astype(BF16).astype(F32)

    q_scr[...] = jnp.transpose(rope(proj[:width])) * (head_dim ** -0.5)
    pad = jnp.zeros((width, k_scr.shape[1] - batch), F32)
    k_scr[...] = jnp.concatenate([rope(proj[width:2 * width]), pad], axis=1)
    v_scr[...] = jnp.concatenate([proj[2 * width:].astype(BF16).astype(F32), pad], axis=1)


def attend_tile(seq0, head_dim, lens, place_k, place_v, q_scr, k_in, v_in, k_new, v_new, after_keys):
    width, cache_len = k_in.shape[1:]
    own_head = (lax.broadcasted_iota(jnp.int32, (HEAD_ROWS, width), 1) // head_dim
                == lax.broadcasted_iota(jnp.int32, (HEAD_ROWS, width), 0))
    lane_row = lax.broadcasted_iota(jnp.int32, (HEAD_ROWS, cache_len), 1)
    scores = []
    for j in range(SEQ_TILE):
        length = lens[seq0 + j]
        k_val = place_k(length, j, k_in[seq0 + j])
        k_new[seq0 + j] = k_val
        q_block = jnp.where(own_head, q_scr[pl.ds(seq0 + j, 1), :], 0.0).astype(BF16)
        scores.append(jnp.where(lane_row <= length, dot_nn(q_block, k_val), MASK_FILL))
    after_keys()
    score = jnp.concatenate(scores, axis=0)
    expo = jnp.exp(score - jnp.max(score, axis=-1, keepdims=True))
    probs = (expo / jnp.sum(expo, axis=-1, keepdims=True)).astype(BF16)
    outs = []
    for j in range(SEQ_TILE):
        v_val = place_v(lens[seq0 + j], j, v_in[seq0 + j])
        v_new[seq0 + j] = v_val
        mixed = dot_nt(probs[j * HEAD_ROWS:(j + 1) * HEAD_ROWS], v_val)
        outs.append(jnp.sum(jnp.where(own_head, mixed, 0.0), axis=0, keepdims=True))
    return jnp.concatenate(outs, axis=0).astype(BF16)


def opening_kernel(tg_size, sizes, lens, lens_row, hidden, attn_gain, mlp_gain, w_qkv, w_o, w_gu, w_dn, k_cache, v_cache,
                   normed, h_out, gains, cos_t, sin_t, gate_buf, up_buf, gate1, qkv0, qkv1, o1, k_first, v_first,
                   k_next, v_next, up_held, dn_held,
                   o_buf, dn_buf, part, slots, mid, hidden_buf, first_norm, attn, q_scr, k_scr, v_scr, own_gain, far_gain,
                   load_sem, gain_send, gain_recv, sum_send, sum_recv, *sems):
    head_dim = sizes[0]
    place = Place(tg_size)
    make = Maker(place, sems, sizes)
    qkv_u = make.gather("qkv", 0, w_qkv, qkv0, BOTH)
    o_u = make.gather("o", 0, w_o, o_buf, BOTH)
    gate_u = make.gather("gate", 0, w_gu, gate_buf, BOTH)
    up_u = make.gather("up", 0, w_gu, up_buf, BOTH)
    dn_u = make.gather("dn", 0, w_dn, dn_buf, BOTH)
    now_u = qkv_u + o_u + gate_u + up_u + dn_u
    next_u = make.gather("qkv", 1, w_qkv, qkv1, HALVES) + make.gather("o", 1, w_o, o1, HALVES)
    late = len(next_u)
    next_u += make.gather("gate", 1, w_gu, gate1, ("other", "owner"))
    crossing = make.cross("up", 1, w_gu, up_held) + make.cross("dn", 1, w_dn, dn_held)
    flow = Flow(now_u, 2)
    sum_o = SumOverTg(place, part.at[0], slots.at[0], mid, (sum_send.at[0], sum_recv.at[0]))
    sum_d = SumOverTg(place, part.at[1], slots.at[1], normed, (sum_send.at[1], sum_recv.at[1]))
    count = slots.shape[2]
    loads = [pltpu.make_async_copy(src, dst, load_sem.at[k]) for k, (src, dst) in enumerate([
        (hidden, hidden_buf), (attn_gain, own_gain.at[0]), (mlp_gain, own_gain.at[1]),
        (k_cache.at[0], k_first), (v_cache.at[0], v_first), (k_cache.at[1], k_next), (v_cache.at[1], v_next)])]

    for copy in loads[:3]:
        copy.start()
    place.barrier(True)
    gain_copies = [
        pltpu.make_async_remote_copy(
            src_ref=src, dst_ref=far_gain.at[k], send_sem=gain_send.at[k], recv_sem=gain_recv.at[k],
            device_id={"pp": place.stage}, device_id_type=MESH) for k, src in enumerate([attn_gain, mlp_gain])]
    for copy in gain_copies:
        copy.start()
    each(qkv_u + o_u, "start")
    each(gate_u + up_u + dn_u + next_u, "start")
    each(crossing, "start")
    for copy in loads[3:5]:
        copy.start()
    half = cos_t.shape[0]
    power = lax.broadcasted_iota(jnp.int32, cos_t.shape, 0).astype(F32) * (-math.log(ROPE_THETA) / half)
    angle = jnp.exp(power) * lens_row[...].astype(F32)
    cos_t[...] = jnp.cos(angle)
    sin_t[...] = jnp.sin(angle)
    flow.through(qkv_u[1], "send")
    for copy in loads[:3] + gain_copies:
        copy.wait()
    first = place.pp == 0
    table = []
    for k in range(2):
        own_row, far_row = own_gain[k].astype(F32), far_gain[k].astype(F32)
        table.append(jnp.where(first, own_row, far_row))
        table.append(jnp.where(first, far_row, own_row))
    for k, row in enumerate(table):
        gains[pl.ds(k, 1), :] = row
    first_norm[...] = norm_rows(hidden_buf[...].astype(F32), table[0])
    flow.through(qkv_u[-1], "relay")
    flow.through(gate_u[0], "send")
    each(qkv_u, "arrive")
    project(qkv0[...], first_norm[...], cos_t[...], sin_t[...], head_dim, q_scr, k_scr, v_scr)
    for copy in loads[3:5]:
        copy.wait()

    lane = lax.broadcasted_iota(jnp.int32, k_first.shape[1:], 1)
    marks = [(gate_u[1], "send"), (gate_u[2], "send"), (gate_u[3], "send"), (up_u[0], "send")]
    for tile, mark in enumerate(marks):
        seq0 = tile * SEQ_TILE
        k_cols, v_cols = k_scr[...].astype(BF16), v_scr[...].astype(BF16)
        put_k = lambda length, j, old: jnp.where(lane == length, k_cols[:, seq0 + j:seq0 + j + 1], old)
        put_v = lambda length, j, old: jnp.where(lane == length, v_cols[:, seq0 + j:seq0 + j + 1], old)
        attn[pl.ds(seq0, SEQ_TILE), :] = attend_tile(
            seq0, head_dim, lens, put_k, put_v, q_scr, k_first, v_first, k_first, v_first, lambda: None)
        flow.through(*mark)

    for copy in loads[5:]:
        copy.start()
    each(o_u, "arrive")
    part[0] = dot_nn(attn[...], o_buf[...])
    sum_o.scatter_start()
    flow.through(dn_u[0], "send")
    own_rows = hidden_buf[pl.ds(pl.multiple_of(place.tg * count, count), count), :]
    h_mid = (own_rows.astype(F32) + sum_o.total()).astype(BF16).astype(F32)
    sum_o.spread_start(norm_rows(h_mid, gains[2:3, :]))
    flow.through(dn_u[-1], "send")
    each(next_u, "send")
    each(gate_u, "arrive")
    sum_o.spread_finish()
    act_in = mid[...]
    gate = jax.nn.silu(dot_nt(act_in, gate_buf[...]))
    flow.through(dn_u[-1], "relay")
    each(up_u, "arrive")
    act = (gate * dot_nt(act_in, up_buf[...])).astype(BF16)
    each(dn_u, "arrive")
    part[1] = dot_nn(act, dn_buf[...])
    sum_d.scatter_start()
    each(next_u[:late], "relay")
    each(next_u[:late // 2], "receive")
    h_new = (h_mid + sum_d.total()).astype(BF16)
    h_out[...] = h_new
    sum_d.spread_start(norm_rows(h_new.astype(F32), gains[1:2, :]))
    each(next_u[late:], "relay")
    each(next_u[late // 2:late], "receive")
    each(now_u, "finish")
    each(next_u[late:], "receive")
    each(crossing, "finish")
    sum_d.spread_finish()
    each(next_u, "arrive")
    each(next_u, "finish")
    for copy in loads[5:]:
        copy.wait()


def attend_kernel(head_dim, lens, normed, w_qkv, cos_t, sin_t, k_in, v_in, w_first, gate, up, gate1, k_first, v_first,
                  k_out, v_out, gen_qkv, gen_gu, attn_out, k_new, v_new, q_scr, k_scr, v_scr, kv_sem, gen_sem):
    ffn = gate.shape[0]
    gens = [pltpu.make_async_copy(src, dst, gen_sem.at[k]) for k, (src, dst) in enumerate([
        (k_first, k_out.at[0]), (v_first, v_out.at[0]), (w_first, gen_qkv.at[0]), (w_qkv, gen_qkv.at[1]),
        (gate, gen_gu.at[0, pl.ds(0, ffn)]), (up, gen_gu.at[0, pl.ds(ffn, ffn)]),
        (gate1, gen_gu.at[1, pl.ds(0, ffn)])])]
    for copy in gens:
        copy.start()
    batch, width = q_scr.shape
    cache_len = k_in.shape[2]
    project(w_qkv[...], normed[...], cos_t[...], sin_t[...], head_dim, q_scr, k_scr, v_scr)
    lane = lax.broadcasted_iota(jnp.int32, (width, cache_len), 1)

    def copy_out(k, i):
        block = pl.ds(i * SEQ_TILE, SEQ_TILE)
        new, out = [(k_new, k_out), (v_new, v_out)][k]
        return pltpu.make_async_copy(new.at[block], out.at[1, block], kv_sem.at[k, i])

    def step(i, carry):
        seq0 = i * SEQ_TILE

        def placer(cols):
            def place(length, j, old):
                moved = pltpu.roll(cols, lax.rem(length - seq0 - j + cache_len, cache_len), 1).astype(BF16)
                return jnp.where(lane == length, moved, old)

            return place

        out = attend_tile(seq0, head_dim, lens, placer(k_scr[...]), placer(v_scr[...]), q_scr, k_in, v_in, k_new, v_new,
                          lambda: copy_out(0, i).start())
        copy_out(1, i).start()
        attn_out[pl.ds(pl.multiple_of(seq0, SEQ_TILE), SEQ_TILE), :] = out
        return carry

    steps = batch // SEQ_TILE
    lax.fori_loop(0, steps, step, 0)
    for i in range(steps):
        copy_out(0, i).wait()
        copy_out(1, i).wait()
    for copy in gens:
        copy.wait()


def last_layer_kernel(tg_size, sizes, attn, h_in, gains, o1, gate1, up_held, dn_held, w_gu, w_dn,
                      hidden_out, up_buf, dn_buf, part, slots, mid, sum_send, sum_recv, *sems):
    place = Place(tg_size)
    make = Maker(place, sems, sizes)
    up_u = make.gather("up", 1, w_gu, up_buf, HALVES, up_held)
    dn_u = make.gather("dn", 1, w_dn, dn_buf, HALVES, dn_held)
    every = up_u + dn_u
    sum_o = SumOverTg(place, part.at[0], slots.at[0], mid, (sum_send.at[0], sum_recv.at[0]))
    sum_d = SumOverTg(place, part.at[1], slots.at[1], hidden_out, (sum_send.at[1], sum_recv.at[1]))

    place.barrier(True)
    each(every, "start")
    part[0] = dot_nn(attn[...], o1[...])
    sum_o.scatter_start()
    each(every, "send")
    each(up_u, "relay")
    h_mid = (h_in[...].astype(F32) + sum_o.total()).astype(BF16).astype(F32)
    sum_o.spread_start(norm_rows(h_mid, gains[3:4, :]))
    each(up_u, "receive")
    each(dn_u, "relay")
    sum_o.spread_finish()
    act_in = mid[...]
    gate = jax.nn.silu(dot_nt(act_in, gate1[...]))
    each(up_u, "arrive")
    act = (gate * dot_nt(act_in, up_buf[...])).astype(BF16)
    each(dn_u, "receive")
    each(dn_u, "arrive")
    part[1] = dot_nn(act, dn_buf[...])
    sum_d.scatter_start()
    each(every, "finish")
    h_new = (h_mid + sum_d.total()).astype(BF16)
    sum_d.spread_start(h_new)
    sum_d.spread_finish()


def store_kernel(up, hidden, prior, gen_gu, hidden_out, sem):
    ffn = up.shape[0]
    copies = [pltpu.make_async_copy(src, dst, sem.at[k]) for k, (src, dst) in enumerate([
        (up, gen_gu.at[1, pl.ds(ffn, ffn)]), (hidden, hidden_out)])]
    for copy in copies:
        copy.start()
    for copy in copies:
        copy.wait()


MIB = 1024 * 1024
OPENING_VMEM, ATTEND_VMEM, LAST_VMEM = 34 * MIB, 34 * MIB, 34 * MIB


def remote_params(collective_id, limit):
    return pltpu.CompilerParams(collective_id=collective_id, has_side_effects=True, vmem_limit_bytes=limit)


def solution(mesh):
    merge = mesh.shape["grp"]
    tg_size = mesh.shape["tg"]
    cache_spec = P(None, ROW_AXES, None, "tg", None)
    in_specs = (P(ROW_AXES, None), P(ROW_AXES), cache_spec, cache_spec,
                P("pp", None), P("pp", TRAIN_AXES, None), P("pp", None, TRAIN_AXES),
                P("pp", None), P("pp", TRAIN_AXES, None), P("pp", None, TRAIN_AXES))
    out_specs = (P(ROW_AXES, None), cache_spec, cache_spec, P(None, "tg", None), P(None, "tg", None))

    def body(hidden_in, seq_lens, k_cache, v_cache, attn_gain, w_qkv, w_o, mlp_gain, w_gate_up, w_down):
        batch, dim = hidden_in.shape
        layers, _, cache_len, kv_loc, head_dim = k_cache.shape
        width = kv_loc * head_dim
        ffn_rows = w_gate_up.shape[1] // 2
        ffn = ffn_rows * merge
        sizes = (head_dim, ffn_rows, merge)
        quarter = batch // tg_size
        w_qkv, w_gate_up = w_qkv[0], w_gate_up[0]
        w_o_t, w_down_t = jnp.transpose(w_o[0]), jnp.transpose(w_down[0])
        flat = lambda cache: jnp.transpose(cache, (0, 1, 3, 4, 2)).reshape(layers, batch, width, cache_len)
        k_flat, v_flat = flat(k_cache), flat(v_cache)
        dma = pltpu.SemaphoreType.DMA
        sds = jax.ShapeDtypeStruct
        layer_kv = sds((batch, width, cache_len), BF16)
        merged_qkv, merged_o, merged_ffn = (sds((3 * width, dim), BF16), sds((width, dim), BF16), sds((ffn, dim), BF16))
        act, held = sds((batch, dim), BF16), sds((ffn_rows, dim), BF16)
        rope = sds((head_dim // 2, batch), F32)
        sum_scratch = [pltpu.VMEM((2, batch, dim), F32), pltpu.VMEM((2, tg_size - 1, quarter, dim), F32),
                       pltpu.VMEM((batch, dim), BF16)]
        sum_sems = [dma((2, 2, tg_size - 1)), dma((2, 2, tg_size - 1))]

        projected = [pltpu.VMEM((batch, width), F32), pltpu.VMEM((width, cache_len), F32),
                     pltpu.VMEM((width, cache_len), F32)]
        on_chip = lambda like: pltpu.VMEM(like.shape, like.dtype)
        off_chip = lambda like: pltpu.HBM(like.shape, like.dtype)
        hbm = lambda *arrays: [pltpu.with_memory_space_constraint(arr, pltpu.HBM) for arr in arrays]
        vmem = lambda *arrays: [pltpu.with_memory_space_constraint(arr, pltpu.VMEM) for arr in arrays]
        shared = [act, sds((quarter, dim), BF16), sds((4, dim), F32), rope, rope, merged_ffn, merged_ffn, merged_ffn,
                  merged_qkv, merged_qkv, merged_o, layer_kv, layer_kv, layer_kv, layer_kv]
        (normed, h_own, gains, cos_t, sin_t, gate0, up0, gate1, qkv0, qkv1, o1, k_first, v_first, k_next, v_next,
         up_held, dn_held) = pl.pallas_call(
            functools.partial(opening_kernel, tg_size, sizes),
            in_specs=[SMEM, VMEM] + [HBM] * 9, out_specs=[VMEM] * 15 + [HBM] * 2,
            out_shape=[on_chip(x) for x in shared] + [off_chip(held)] * 2,
            scratch_shapes=[pltpu.VMEM((width, dim), BF16), pltpu.VMEM((ffn, dim), BF16)] + sum_scratch + [
                pltpu.VMEM((batch, dim), BF16), pltpu.VMEM((batch, dim), BF16), pltpu.VMEM((batch, width), BF16)]
            + projected + [pltpu.VMEM((2, 1, dim), BF16), pltpu.VMEM((2, 1, dim), BF16),
                           dma((7,)), dma((2,)), dma((2,))] + sum_sems + gather_sems(34),
            compiler_params=remote_params(1, OPENING_VMEM), name="opening",
        )(seq_lens, seq_lens.reshape(1, batch), *hbm(hidden_in, attn_gain, mlp_gain, w_qkv, w_o_t, w_gate_up, w_down_t,
                                                     k_flat, v_flat))

        cache_shape = off_chip(k_flat)
        k_out, v_out, gen_qkv, gen_gate_up, attn = pl.pallas_call(
            functools.partial(attend_kernel, head_dim),
            in_specs=[SMEM] + [VMEM] * 12, out_specs=[HBM] * 4 + [VMEM],
            out_shape=[cache_shape, cache_shape, pltpu.HBM((layers, 3 * width, dim), BF16),
                       pltpu.HBM((layers, 2 * ffn, dim), BF16), pltpu.VMEM((batch, width), BF16)],
            scratch_shapes=[pltpu.VMEM(layer_kv.shape, BF16)] * 2 + projected + [
                dma((2, batch // SEQ_TILE)), dma((7,))],
            compiler_params=pltpu.CompilerParams(vmem_limit_bytes=ATTEND_VMEM), name="attend",
        )(seq_lens, *vmem(normed, qkv1, cos_t, sin_t, k_next, v_next, qkv0, gate0, up0, gate1, k_first, v_first))

        hidden, up1 = pl.pallas_call(
            functools.partial(last_layer_kernel, tg_size, sizes),
            in_specs=[VMEM] * 5 + [HBM] * 4, out_specs=[VMEM] * 2,
            out_shape=[on_chip(act), on_chip(merged_ffn)],
            scratch_shapes=[pltpu.VMEM((ffn, dim), BF16)] + sum_scratch + sum_sems + gather_sems(8),
            compiler_params=remote_params(2, LAST_VMEM), name="layer_1",
        )(*vmem(attn, h_own, gains, o1, gate1), *hbm(up_held, dn_held, w_gate_up, w_down_t))

        gen_gate_up, hidden = pl.pallas_call(
            store_kernel, in_specs=[VMEM, VMEM, HBM], out_specs=[HBM, HBM],
            out_shape=[pltpu.HBM(gen_gate_up.shape, BF16), off_chip(act)],
            scratch_shapes=[dma((2,))], input_output_aliases={2: 0}, name="store",
        )(*vmem(up1, hidden), gen_gate_up)

        unflat = lambda cache: jnp.transpose(
            cache.reshape(layers, batch, kv_loc, head_dim, cache_len), (0, 1, 4, 2, 3))
        return hidden, unflat(k_out), unflat(v_out), gen_qkv, gen_gate_up

    return jax.shard_map(body, mesh=mesh, in_specs=in_specs, out_specs=out_specs, check_vma=False)
```
